256 devices in a mesh: fsdp: 8 (over x, y_hi), seq: 32 (over y_lo, z, core).
Axes of the slice: x: 4, y: 4 (y_hi: 2, y_lo: 2; y = y_hi * 2 + y_lo), z: 8, core: 2. Of those that a mesh axis runs over, the one named last changes fastest.
Arguments:
- q_next: bfloat16 [32768, 4096], P(('fsdp', 'seq')), may hold values from -9 to 9
- k_next: bfloat16 [32768, 1024], P(('fsdp', 'seq')), may hold values from -4 to 4
- v_next: bfloat16 [32768, 1024], P(('fsdp', 'seq')), may hold values from -6 to 6
- seg_next: int32 [8, 4096], P('fsdp'), may hold values from 0 to 15, never falling along the last dimension, each value on 1 to 512 neighbouring positions
- q_prev: bfloat16 [32768, 4096], P(('fsdp', 'seq')), may hold values from -9 to 9
- k_prev: bfloat16 [32768, 1024], P(('fsdp', 'seq')), may hold values from -4 to 4
- v_prev: bfloat16 [32768, 1024], P(('fsdp', 'seq')), may hold values from -6 to 6
- seg_prev: int32 [8, 4096], P('fsdp'), may hold values from 0 to 15, never falling along the last dimension, each value on 1 to 512 neighbouring positions
- upstream: bfloat16 [32768, 4096], P(('fsdp', 'seq')), may hold values from -6 to 6
- flags: int32 [8, 4096], P('fsdp', 'seq'), may hold values from 0 to 1
Outputs:
- attn_next: bfloat16 [32768, 4096], P(('fsdp', 'seq'))
- grad_q: bfloat16 [32768, 4096], P(('fsdp', 'seq'))
- grad_k: bfloat16 [32768, 1024], P(('fsdp', 'seq'))
- grad_v: bfloat16 [32768, 1024], P(('fsdp', 'seq'))
The draws below stay inside these ranges and needn't reach their ends.
Inputs may be any that keep to these rules, and one draw needn't show every extreme that they name: `seg_next`: within each sequence the ids never fall and each id covers at most 512 consecutive positions; some id covers exactly 512. `seg_prev`: within each sequence the ids never fall and each id covers at most 512 consecutive positions; some id covers exactly 512.
All inputs are finite; a program needn't handle non-finite values.
Results may differ from the reference program's by a relative error of at most 0.0067.
Values may be sent and summed in bfloat16 or wider, within the bound.
A program may use at most 128 MiB of HBM per device.

```python
import math
import jax
import jax.numpy as jnp
import numpy as np
from jax import lax

HEADS = 32
KV_HEADS = 8
HEAD_DIM = 128
TOK_DEV = 128
BATCH = 8
SEQ = 4096
TOKENS = 32768
SEG_MOST = 512
BLOCK = 512


def draw_pair(key, marker):
    key = jax.random.fold_in(key, marker)
    query_key, keys_key = jax.random.split(key, 2)
    queries = jnp.clip(jax.random.normal(query_key, (TOKENS, HEADS * HEAD_DIM), jnp.float32), -4.0, 4.0)
    keys_all = jnp.clip(jax.random.normal(keys_key, (TOKENS, KV_HEADS * HEAD_DIM), jnp.float32), -4.0, 4.0)
    return (queries.astype(jnp.bfloat16), keys_all.astype(jnp.bfloat16))


def draw_q_next(key, part):
    return draw_pair(key, 11)[0]


def draw_k_next(key, part):
    return draw_pair(key, 11)[1]


def draw_q_prev(key, part):
    return draw_pair(key, 23)[0]


def draw_k_prev(key, part):
    return draw_pair(key, 23)[1]


def draw_flags(key, part):
    key = jax.random.fold_in(key, 37)
    level_key, dice_key = jax.random.split(key)
    levels = jax.random.randint(level_key, (BATCH, SEQ // TOK_DEV), 4, 11)
    limits = jnp.left_shift(jnp.ones_like(levels), levels)
    limit_rows = jnp.repeat(limits, TOK_DEV, axis=1)
    dice = jax.random.randint(dice_key, (BATCH, SEQ), 0, 1024)
    return (dice < limit_rows).astype(jnp.int32)


def block_scale(rng, extent, shards, low, top_value):
    def one(axis_at, blocks):
        draws = jax.random.uniform(jax.random.fold_in(jax.random.fold_in(rng, 6), axis_at), (blocks,), jnp.float32, low / len(shards), top_value / len(shards))
        return jnp.repeat(jnp.exp(draws), extent[axis_at] // blocks).reshape((-1,) + (1,) * (len(extent) - axis_at - 1))

    factor_of = one(*shards[0])
    for cut in shards[1:]:
        factor_of = factor_of * one(*cut)
    return factor_of


def length_profile(count, total, most, lean):
    portions = [(1 << 20) // math.isqrt(grade ** lean) + 1 for grade in range(2, count + 1)]
    surplus, given = total - most - (count - 1), [1] * (count - 1)
    while surplus > 0:
        candidates = [i for i in range(count - 1) if given[i] < most]
        whole, left = sum([portions[i] for i in candidates]), surplus
        for i in candidates:
            addition = min(most - given[i], max(1, left * portions[i] // whole), surplus)
            given[i] = given[i] + addition
            surplus = surplus - addition
    return np.array([most] + given)


def ragged_sizes(key, count, total, most, lean):
    if count == 2:
        one = jax.random.randint(key, (), max(1, total - most), min(most, total - 1) + 1)
        return jnp.stack([one, total - one])
    tallies = jnp.asarray(length_profile(count, total, most, lean), jnp.int32)
    pairs = (count - 1) // 2
    giver, taker = tallies[1:1 + 2 * pairs:2], tallies[2:2 + 2 * pairs:2]
    slack = jnp.minimum(giver - 1, most - taker)
    shifted = jax.random.randint(jax.random.fold_in(key, 1), (pairs,), 0, 1 << 20) % (slack + 1)
    tallies = tallies.at[1:1 + 2 * pairs:2].set(giver - shifted).at[2:2 + 2 * pairs:2].set(taker + shifted)
    return tallies[jax.random.permutation(jax.random.fold_in(key, 2), count)]


def noise(rng, extent, deviation, limit, pieces=(), kind=jnp.bfloat16):
    gain = block_scale(rng, extent, pieces, -0.22, 0.18) if pieces else 1.0
    entries = jax.random.normal(rng, extent, jnp.float32) * deviation * gain
    return jnp.minimum(jnp.maximum(entries, -limit), limit).astype(kind)


def setup_inputs(seed: int = 0) -> dict:
    arg_keys = jax.random.split(jax.random.key(seed), 11)
    q_next = draw_q_next(jax.random.fold_in(arg_keys[10], 71), 0)
    k_next = draw_k_next(jax.random.fold_in(arg_keys[10], 71), 0)
    v_next = noise(arg_keys[2], (TOKENS, KV_HEADS * HEAD_DIM), 1.0, 6.0, ((0, 256),))
    seg_next = jax.vmap(lambda own: jnp.searchsorted(jnp.cumsum(ragged_sizes(own, 2 * SEQ // SEG_MOST, SEQ, SEG_MOST, 1)), jnp.arange(SEQ), side="right"))(jax.random.split(arg_keys[3], BATCH)).reshape((BATCH, SEQ)).astype(jnp.int32)
    q_prev = draw_q_prev(jax.random.fold_in(arg_keys[10], 71), 0)
    k_prev = draw_k_prev(jax.random.fold_in(arg_keys[10], 71), 0)
    v_prev = noise(arg_keys[6], (TOKENS, KV_HEADS * HEAD_DIM), 1.0, 6.0, ((0, 256),))
    seg_prev = jax.vmap(lambda own: jnp.searchsorted(jnp.cumsum(ragged_sizes(own, 2 * SEQ // SEG_MOST, SEQ, SEG_MOST, 1)), jnp.arange(SEQ), side="right"))(jax.random.split(arg_keys[7], BATCH)).reshape((BATCH, SEQ)).astype(jnp.int32)
    upstream = noise(arg_keys[8], (TOKENS, HEADS * HEAD_DIM), 1.0, 6.0, ((0, 256),))
    flags = draw_flags(jax.random.fold_in(arg_keys[10], 71), 0)
    return dict(q_next=q_next, k_next=k_next, v_next=v_next, seg_next=seg_next, q_prev=q_prev, k_prev=k_prev, v_prev=v_prev, seg_prev=seg_prev, upstream=upstream, flags=flags)


def narrow(values):
    return lax.optimization_barrier(values.astype(jnp.bfloat16)).astype(jnp.float32)


def masked_probs(q_block, k_window, q_pos, k_pos, q_seg, k_seg):
    scale_factor = HEAD_DIM ** -0.5
    scores = jnp.einsum('qhd,khd->hqk', q_block.astype(jnp.float32), k_window.astype(jnp.float32)) * scale_factor
    keep_mask = (k_seg[None, :] == q_seg[:, None]) & (k_pos[None, :] <= q_pos[:, None])
    scores = jnp.where(keep_mask[None], scores, -1e30)
    row_max = jnp.max(scores, axis=-1, keepdims=True)
    expo_vals = jnp.exp(scores - row_max)
    return expo_vals / jnp.sum(expo_vals, axis=-1, keepdims=True)


def block_window(seq_ids, block_start):
    padded = jnp.concatenate([jnp.full((SEG_MOST,), -1, jnp.int32), seq_ids.astype(jnp.int32)])
    q_seg = lax.dynamic_slice_in_dim(seq_ids.astype(jnp.int32), block_start, BLOCK)
    k_seg = lax.dynamic_slice_in_dim(padded, block_start, SEG_MOST + BLOCK)
    q_pos = block_start + jnp.arange(BLOCK, dtype=jnp.int32)
    k_pos = block_start - SEG_MOST + jnp.arange(SEG_MOST + BLOCK, dtype=jnp.int32)
    return q_pos, k_pos, q_seg, k_seg


def pad_front(array):
    return jnp.concatenate([jnp.zeros((SEG_MOST,) + array.shape[1:], array.dtype), array], axis=0)


def forward_heads(q_heads, k_heads, v_heads, seq_ids):
    k_padded = pad_front(k_heads)
    v_padded = pad_front(v_heads)

    def block_step(block_idx, output):
        block_start = (block_idx * BLOCK).astype(jnp.int32)
        q_pos, k_pos, q_seg, k_seg = block_window(seq_ids, block_start)
        q_block = lax.dynamic_slice_in_dim(q_heads, block_start, BLOCK, 0)
        k_window = lax.dynamic_slice_in_dim(k_padded, block_start, SEG_MOST + BLOCK, 0)
        v_window = lax.dynamic_slice_in_dim(v_padded, block_start, SEG_MOST + BLOCK, 0)
        soft_probs = masked_probs(q_block, k_window, q_pos, k_pos, q_seg, k_seg)
        result = jnp.einsum('hqk,khd->qhd', narrow(soft_probs), v_window.astype(jnp.float32)).astype(jnp.bfloat16)
        return lax.dynamic_update_slice_in_dim(output, result, block_start, 0)

    return lax.fori_loop(0, SEQ // BLOCK, block_step, jnp.zeros(q_heads.shape, jnp.bfloat16))


def backward_heads(q_heads, k_heads, v_heads, d_heads, seq_ids):
    k_padded = pad_front(k_heads)
    v_padded = pad_front(v_heads)
    scale_factor = HEAD_DIM ** -0.5

    def block_step(block_idx, carry):
        grad_qh, k_grads, v_grads = carry
        block_start = (block_idx * BLOCK).astype(jnp.int32)
        q_pos, k_pos, q_seg, k_seg = block_window(seq_ids, block_start)
        q_block = lax.dynamic_slice_in_dim(q_heads, block_start, BLOCK, 0).astype(jnp.float32)
        d_block = lax.dynamic_slice_in_dim(d_heads, block_start, BLOCK, 0).astype(jnp.float32)
        k_window = lax.dynamic_slice_in_dim(k_padded, block_start, SEG_MOST + BLOCK, 0).astype(jnp.float32)
        v_window = lax.dynamic_slice_in_dim(v_padded, block_start, SEG_MOST + BLOCK, 0).astype(jnp.float32)
        soft_probs = masked_probs(q_block, k_window, q_pos, k_pos, q_seg, k_seg)
        d_probs = jnp.einsum('qhd,khd->hqk', d_block, v_window)
        row_delta = jnp.sum(soft_probs * d_probs, axis=-1, keepdims=True)
        d_scores = narrow(soft_probs * (d_probs - row_delta) * scale_factor)
        q_grad = jnp.einsum('hqk,khd->qhd', d_scores, k_window).astype(jnp.bfloat16)
        k_term = jnp.einsum('hqk,qhd->khd', d_scores, q_block)
        v_term = jnp.einsum('hqk,qhd->khd', narrow(soft_probs), d_block)
        grad_qh = lax.dynamic_update_slice_in_dim(grad_qh, q_grad, block_start, 0)
        k_old = lax.dynamic_slice_in_dim(k_grads, block_start, SEG_MOST + BLOCK, 0)
        v_old = lax.dynamic_slice_in_dim(v_grads, block_start, SEG_MOST + BLOCK, 0)
        k_grads = lax.dynamic_update_slice_in_dim(k_grads, k_old + k_term, block_start, 0)
        v_grads = lax.dynamic_update_slice_in_dim(v_grads, v_old + v_term, block_start, 0)
        return grad_qh, k_grads, v_grads

    buffer_shape = (SEG_MOST + SEQ,) + q_heads.shape[1:]
    start_carry = (jnp.zeros(q_heads.shape, jnp.bfloat16), jnp.zeros(buffer_shape, jnp.float32), jnp.zeros(buffer_shape, jnp.float32))
    grad_qh, k_grads, v_grads = lax.fori_loop(0, SEQ // BLOCK, block_step, start_carry)
    return grad_qh, k_grads[SEG_MOST:], v_grads[SEG_MOST:]


def reference(q_next, k_next, v_next, seg_next, q_prev, k_prev, v_prev, seg_prev, upstream, flags):
    group_size = HEADS // KV_HEADS

    def query_heads(array):
        return array.reshape(BATCH, SEQ, HEADS, HEAD_DIM)

    def shared_heads(array):
        return jnp.repeat(array.reshape(BATCH, SEQ, KV_HEADS, HEAD_DIM), group_size, axis=2)

    def group_sum(array):
        summed = jnp.sum(array.reshape(TOKENS, KV_HEADS, group_size, HEAD_DIM).astype(jnp.float32), axis=2)
        return summed.astype(jnp.bfloat16).reshape(TOKENS, KV_HEADS * HEAD_DIM)

    attn = lax.map(lambda members: forward_heads(*members), (query_heads(q_next), shared_heads(k_next), shared_heads(v_next), seg_next))
    attn_next = attn.reshape(TOKENS, HEADS * HEAD_DIM)
    flag_total = jnp.sum(flags.astype(jnp.float32))
    weight = flags.reshape(TOKENS, 1).astype(jnp.float32) * (TOKENS / jnp.maximum(flag_total, 1.0))
    cotangent = (upstream.astype(jnp.float32) * weight).astype(jnp.bfloat16)
    grads = lax.map(lambda members: backward_heads(*members), (query_heads(q_prev), shared_heads(k_prev), shared_heads(v_prev), query_heads(cotangent), seg_prev))
    grad_q = grads[0].reshape(TOKENS, HEADS * HEAD_DIM)
    grad_k = group_sum(grads[1])
    grad_v = group_sum(grads[2])
    return attn_next, grad_q, grad_k, grad_v
```

```python
import functools
import math

import jax
import jax.numpy as jnp
from jax import lax
from jax.experimental import pallas as pl
from jax.experimental.pallas import tpu as pltpu
from jax.sharding import PartitionSpec as P

HEAD_DIM = 128
GROUP = 4
BLOCKS = 5
AHEAD = 2
LAG = 4
MESH = pl.DeviceIdType.MESH
F32 = jnp.float32
BF16 = jnp.bfloat16


def dot(a, b, dims):
    return lax.dot_general(a, b, (dims, ((), ())), preferred_element_type=F32)


def column_of(row):
    return jnp.transpose(jnp.broadcast_to(row, (128, row.shape[1])))


def kernel(
    sizes,
    q_next, k_next, v_next, seg_next, q_prev, k_prev, v_prev, seg_prev, upstream, flags,
    attn_out, gq_out, gk_out, gv_out,
    own, near, far, side, side_grads, side_recv, grads, far_send, far_recv, near_send, near_recv,
    q_prev_v, up_v, q_next_v, attn_v, gq_v, gk_v, gv_v, dq_t, bias, count_send, count_recv,
    load_sem, array_sem, out_sem, send_sem, recv_sem, gsend_sem, grecv_sem, csend_sem, crecv_sem,
):
    kv_heads, n_fsdp, n_seq = sizes
    chunks = 2 * kv_heads
    width = GROUP * HEAD_DIM
    seq_at = lax.axis_index("seq")
    fsdp_at = lax.axis_index("fsdp")
    core = seq_at % 2
    ahead_at = (seq_at + 2) % n_seq
    behind_at = (seq_at + n_seq - 2) % n_seq
    side_at = seq_at + 1 - 2 * core
    scale = HEAD_DIM ** -0.5

    partners = []
    step = 1
    while step < n_seq:
        partners.append({"seq": seq_at + step - 2 * step * ((seq_at // step) % 2)})
        step *= 2
    step = 1
    while step < n_fsdp:
        partners.append({"fsdp": fsdp_at + step - 2 * step * ((fsdp_at // step) % 2)})
        step *= 2
    rounds = len(partners)

    def remote(src, dst, sems, at, device):
        return pltpu.make_async_remote_copy(
            src_ref=src, dst_ref=dst, send_sem=sems[0].at[at], recv_sem=sems[1].at[at],
            device_id=device, device_id_type=MESH,
        )

    links = (send_sem, recv_sem)
    glinks = (gsend_sem, grecv_sem)

    def own_ahead(t):
        return remote(own.at[t], near.at[t], links, (0, t), {"seq": ahead_at})

    def near_ahead(t):
        return remote(near.at[t], far.at[t], links, (1, t), {"seq": ahead_at})

    def own_side(t):
        return remote(own.at[t], side.at[0, t], links, (2, t), {"seq": side_at})

    def near_side(t):
        return remote(near.at[t], side.at[1, t], links, (3, t), {"seq": side_at})

    def far_side(t):
        return remote(far.at[t], side.at[2, t], links, (4, t), {"seq": side_at})

    def grads_side(t):
        return remote(side_grads.at[t], side_recv.at[t], glinks, (0, t), {"seq": side_at})

    def far_back(t):
        return remote(far_send.at[t], far_recv.at[t], glinks, (1, t), {"seq": behind_at})

    def near_back(t):
        return remote(near_send.at[t], near_recv.at[t], glinks, (2, t), {"seq": behind_at})

    def count_to(r):
        return remote(count_send.at[r], count_recv.at[r], (csend_sem, crecv_sem), r, partners[r])

    def load(t, which):
        k_from, v_from = (k_prev, v_prev) if t < kv_heads else (k_next, v_next)
        src = (k_from, v_from)[which]
        columns = slice((t % kv_heads) * HEAD_DIM, (t % kv_heads + 1) * HEAD_DIM)
        return pltpu.make_async_copy(src.at[:, columns], own.at[t, which], load_sem.at[t, which])

    def wait_load(t):
        for which, src in enumerate((k_prev, v_prev)):
            pltpu.make_async_copy(
                src.at[:, 0:HEAD_DIM], own.at[t, which], load_sem.at[t, which]
            ).wait()

    def columns_of(g, count=GROUP):
        return pl.ds(pl.multiple_of(g * (count * HEAD_DIM), HEAD_DIM), count * HEAD_DIM)

    def attn_copy(g):
        return pltpu.make_async_copy(
            attn_v.at[:, columns_of(g)], attn_out.at[:, columns_of(g)], out_sem.at[0, g]
        )

    def gq_copy(g):
        return pltpu.make_async_copy(
            gq_v.at[:, columns_of(g)], gq_out.at[:, columns_of(g)], out_sem.at[1, g]
        )

    def gkv_copy(which, g):
        src, dst = ((gk_v, gk_out), (gv_v, gv_out))[which]
        return pltpu.make_async_copy(
            src.at[:, columns_of(g, 1)], dst.at[:, columns_of(g, 1)], out_sem.at[2 + which, g]
        )

    for t in range(chunks):
        load(t, 0).start()
        load(t, 1).start()
    arrays = ((q_prev, q_prev_v), (upstream, up_v), (q_next, q_next_v))
    array_copies = [
        pltpu.make_async_copy(src, dst, array_sem.at[i]) for i, (src, dst) in enumerate(arrays)
    ]
    for copy in array_copies:
        copy.start()

    barrier = pltpu.get_barrier_semaphore()
    peers = [{"seq": ahead_at}, {"seq": behind_at}] + partners
    for peer in peers:
        pl.semaphore_signal(barrier, inc=1, device_id=peer, device_id_type=MESH)

    count_send[0] = jnp.broadcast_to(
        jnp.sum(flags[...].astype(F32), axis=1, keepdims=True), count_send.shape[1:]
    )
    pl.semaphore_wait(barrier, len(peers))

    for t in range(AHEAD):
        wait_load(t)
        own_ahead(t).start()
        own_side(t).start()

    rows_at = lax.broadcasted_iota(jnp.int32, (HEAD_DIM, HEAD_DIM), 0)
    lanes_at = lax.broadcasted_iota(jnp.int32, (HEAD_DIM, HEAD_DIM), 1)
    for m, seg in enumerate((seg_prev, seg_next)):
        def ids_at(index, seg=seg):
            return seg[:, pl.ds(pl.multiple_of(index * HEAD_DIM, HEAD_DIM), HEAD_DIM)].astype(F32)

        q_ids = ids_at(seq_at)
        for d in range(BLOCKS):
            k_ids = column_of(ids_at((seq_at + n_seq - d) % n_seq))
            keep = k_ids == q_ids
            if d == 0:
                keep = keep & (rows_at <= lanes_at)
                block_bias = jnp.where(keep, 0.0, -1e30)
            else:
                block_bias = jnp.where(keep, 0.0, -1e30)
                block_bias = jnp.where(seq_at >= d, block_bias, -1e30)
            bias[m, d * HEAD_DIM : (d + 1) * HEAD_DIM, :] = block_bias

    def window(w, which):
        return jnp.concatenate(
            [own[w, which], side[1 - core, w, which], near[w, which],
             side[2 - core, w, which], far[w, which]],
            axis=0,
        )

    def stacked(ref, g, first, count):
        return jnp.concatenate(
            [
                ref[:, pl.ds(pl.multiple_of(g * width + j * HEAD_DIM, HEAD_DIM), HEAD_DIM)]
                for j in range(first, first + count)
            ],
            axis=0,
        )

    def expo(k_all, q_part, m):
        pair = bias[m]
        scores = dot(k_all, q_part, ((1,), (1,))) + jnp.concatenate([pair, pair], axis=1)
        top = jnp.max(scores, axis=0, keepdims=True)
        values = jnp.exp2((scores - top) * (scale * math.log2(math.e)))
        return values, 1.0 / jnp.sum(values, axis=0, keepdims=True)

    def backward(w):
        k_all, v_all = window(w, 0), window(w, 1)
        k_turned = jnp.transpose(k_all)
        flag_row = flags[...].astype(F32)
        flag_pair = jnp.concatenate([flag_row, flag_row], axis=1)
        dk = dv = None
        for half in range(2):
            q_part = stacked(q_prev_v, w, 2 * half, 2)
            u_part = stacked(up_v, w, 2 * half, 2)
            values, inverse = expo(k_all, q_part, 0)
            d_probs = dot(v_all, u_part, ((1,), (1,)))
            row_delta = jnp.sum(values * d_probs, axis=0, keepdims=True) * inverse
            probs = values * (inverse * flag_pair)
            d_scores = (probs * (d_probs - row_delta)).astype(BF16)
            dq_t[w, :, half * 256 : (half + 1) * 256] = dot(k_turned, d_scores, ((1,), (0,)))
            dk_part = dot(d_scores, q_part, ((1,), (0,)))
            dv_part = dot(probs.astype(BF16), u_part, ((1,), (0,)))
            dk = dk_part if dk is None else dk + dk_part
            dv = dv_part if dv is None else dv + dv_part
        for which, total in enumerate((dk, dv)):
            for d in range(BLOCKS):
                block = total[d * HEAD_DIM : (d + 1) * HEAD_DIM]
                if d % 2:
                    side_grads[w, d // 2, which] = block.astype(BF16)
                else:
                    grads[w, d // 2, which] = block

    def forward(w):
        g = w - kv_heads
        k_all, v_turned = window(w, 0), jnp.transpose(window(w, 1))
        for half in range(2):
            values, inverse = expo(k_all, stacked(q_next_v, g, 2 * half, 2), 1)
            mixed = dot(v_turned, values.astype(BF16), ((1,), (0,))) * inverse
            for j in range(2):
                at = pl.multiple_of(g * width + (2 * half + j) * HEAD_DIM, HEAD_DIM)
                attn_v[:, pl.ds(at, HEAD_DIM)] = jnp.transpose(
                    mixed[:, j * HEAD_DIM : (j + 1) * HEAD_DIM]
                ).astype(BF16)

    def factor_row():
        total = count_send[rounds, 0:1, :]
        return (HEAD_DIM * n_fsdp * n_seq) / jnp.maximum(total, 1.0)

    def finish_q(g):
        gain = factor_row() * scale
        for j in range(GROUP):
            at = pl.multiple_of(g * width + j * HEAD_DIM, HEAD_DIM)
            turned = jnp.transpose(dq_t[g, :, j * HEAD_DIM : (j + 1) * HEAD_DIM])
            gq_v[:, pl.ds(at, HEAD_DIM)] = (turned * gain).astype(BF16)

    def take_side(w):
        for part in range(2):
            grads[w, core + part] = grads[w, core + part] + side_recv[w, part].astype(F32)
        far_send[w] = grads[w, 2].astype(BF16)

    def take_far(w):
        near_send[w] = (grads[w, 1] + far_recv[w].astype(F32)).astype(BF16)

    def take_near(w):
        total = grads[w, 0] + near_recv[w].astype(F32)
        gain = factor_row()
        gk_v[:, columns_of(w, 1)] = (total[0] * (gain * scale)).astype(BF16)
        gv_v[:, columns_of(w, 1)] = (total[1] * gain).astype(BF16)

    def during(t, first, count):
        return pl.when((t >= first) & (t < first + count))

    for copy in array_copies:
        copy.wait()

    def one_step(t, carry):
        @during(t, 0, chunks - AHEAD)
        def _():
            wait_load(t + AHEAD)
            own_ahead(t + AHEAD).start()
            own_side(t + AHEAD).start()

        @during(t, 0, chunks)
        def _():
            own_ahead(t).wait_recv()
            near_ahead(t).start()
            near_side(t).start()

        @during(t, LAG - 1, chunks)
        def _():
            near_ahead(t - LAG + 1).wait_recv()
            far_side(t - LAG + 1).start()

        @during(t, LAG + 1, kv_heads)
        def _():
            grads_side(t - LAG - 1).start()

        @during(t, LAG + 2, kv_heads)
        def _():
            grads_side(t - LAG - 2).wait_recv()
            take_side(t - LAG - 2)

        @during(t, LAG + 4, kv_heads)
        def _():
            far_back(t - LAG - 4).wait_recv()
            take_far(t - LAG - 4)

        for r in range(1, rounds + 1):
            @pl.when(t == r)
            def _(r=r):
                count_to(r - 1).wait_recv()
                count_send[r] = count_send[r - 1] + count_recv[r - 1]

        @during(t, LAG + 6, kv_heads)
        def _():
            near_back(t - LAG - 6).wait_recv()
            take_near(t - LAG - 6)
            gkv_copy(0, t - LAG - 6).start()
            gkv_copy(1, t - LAG - 6).start()

        @during(t, LAG, chunks)
        def _():
            w = t - LAG
            own_side(w).wait_recv()
            near_side(w).wait_recv()
            far_side(w).wait_recv()

        @during(t, LAG, kv_heads)
        def _():
            backward(t - LAG)

        @during(t, LAG + kv_heads, kv_heads)
        def _():
            forward(t - LAG)
            attn_copy(t - LAG - kv_heads).start()

        @during(t, LAG + kv_heads, kv_heads)
        def _():
            finish_q(t - LAG - kv_heads)
            gq_copy(t - LAG - kv_heads).start()

        @during(t, LAG + 2, kv_heads)
        def _():
            far_back(t - LAG - 2).start()

        @during(t, LAG + 4, kv_heads)
        def _():
            near_back(t - LAG - 4).start()

        for r in range(rounds):
            @pl.when(t == r)
            def _(r=r):
                count_to(r).start()

        return carry

    steps = max(chunks + LAG, kv_heads + LAG + 6, rounds + 1)
    lax.fori_loop(0, steps, one_step, 0)

    def drain(t, carry):
        own_ahead(t).wait_send()
        near_ahead(t).wait_send()
        own_side(t).wait_send()
        near_side(t).wait_send()
        far_side(t).wait_send()
        return carry

    lax.fori_loop(0, chunks, drain, 0)

    def drain_back(g, carry):
        grads_side(g).wait_send()
        far_back(g).wait_send()
        near_back(g).wait_send()
        attn_copy(g).wait()
        gq_copy(g).wait()
        gkv_copy(0, g).wait()
        gkv_copy(1, g).wait()
        return carry

    lax.fori_loop(0, kv_heads, drain_back, 0)
    for r in range(rounds):
        count_to(r).wait_send()


def body(n_fsdp, n_seq, *args):
    q, k = args[0], args[1]
    rows = q.shape[0]
    kv_heads = k.shape[1] // HEAD_DIM
    chunks = 2 * kv_heads
    width = q.shape[1]
    rounds = int(math.log2(n_fsdp * n_seq))
    tile = (2, HEAD_DIM, HEAD_DIM)
    anywhere = pl.BlockSpec(memory_space=pl.ANY)
    vmem = pl.BlockSpec(memory_space=pltpu.VMEM)
    dma = pltpu.SemaphoreType.DMA
    return pl.pallas_call(
        functools.partial(kernel, (kv_heads, n_fsdp, n_seq)),
        out_shape=(
            jax.ShapeDtypeStruct(q.shape, BF16),
            jax.ShapeDtypeStruct(q.shape, BF16),
            jax.ShapeDtypeStruct(k.shape, BF16),
            jax.ShapeDtypeStruct(k.shape, BF16),
        ),
        in_specs=[
            anywhere, anywhere, anywhere, vmem, anywhere, anywhere, anywhere, vmem, anywhere, vmem,
        ],
        out_specs=(anywhere,) * 4,
        scratch_shapes=[
            pltpu.VMEM((chunks,) + tile, BF16),
            pltpu.VMEM((chunks,) + tile, BF16),
            pltpu.VMEM((chunks,) + tile, BF16),
            pltpu.VMEM((3, chunks) + tile, BF16),
            pltpu.VMEM((kv_heads, 2) + tile, BF16),
            pltpu.VMEM((kv_heads, 2) + tile, BF16),
            pltpu.VMEM((kv_heads, 3) + tile, F32),
            pltpu.VMEM((kv_heads,) + tile, BF16),
            pltpu.VMEM((kv_heads,) + tile, BF16),
            pltpu.VMEM((kv_heads,) + tile, BF16),
            pltpu.VMEM((kv_heads,) + tile, BF16),
            pltpu.VMEM((rows, width), BF16),
            pltpu.VMEM((rows, width), BF16),
            pltpu.VMEM((rows, width), BF16),
            pltpu.VMEM((rows, width), BF16),
            pltpu.VMEM((rows, width), BF16),
            pltpu.VMEM(k.shape, BF16),
            pltpu.VMEM(k.shape, BF16),
            pltpu.VMEM((kv_heads, HEAD_DIM, GROUP * HEAD_DIM), F32),
            pltpu.VMEM((2, BLOCKS * HEAD_DIM, HEAD_DIM), F32),
            pltpu.VMEM((rounds + 1, 8, 128), F32),
            pltpu.VMEM((rounds, 8, 128), F32),
            dma((chunks, 2)),
            dma((3,)),
            dma((4, kv_heads)),
            dma((5, chunks)),
            dma((5, chunks)),
            dma((3, kv_heads)),
            dma((3, kv_heads)),
            dma((rounds,)),
            dma((rounds,)),
        ],
        compiler_params=pltpu.CompilerParams(
            collective_id=0, has_side_effects=True, vmem_limit_bytes=60 * 1024 * 1024
        ),
    )(*args)


def solution(mesh):
    both = P(("fsdp", "seq"), None)
    ids = P("fsdp", None)
    return jax.shard_map(
        functools.partial(body, mesh.shape["fsdp"], mesh.shape["seq"]),
        mesh=mesh,
        in_specs=(both, both, both, ids, both, both, both, ids, both, P("fsdp", "seq")),
        out_specs=(both,) * 4,
        check_vma=False,
    )
```

```python
import functools
import math

import jax
import jax.numpy as jnp
from jax import lax
from jax.experimental import pallas as pl
from jax.experimental.pallas import tpu as pltpu
from jax.sharding import PartitionSpec as P

HEAD_DIM = 128
GROUP = 4
BLOCKS = 5
AHEAD = 2
COUNT_STEPS = 5
LAG = 4
MESH = pl.DeviceIdType.MESH
F32 = jnp.float32
BF16 = jnp.bfloat16


def dot(a, b, dims):
    return lax.dot_general(a, b, (dims, ((), ())), preferred_element_type=F32)


def column_of(row):
    return jnp.transpose(jnp.broadcast_to(row, (128, row.shape[1])))


def kernel(
    sizes,
    q_next, k_next, v_next, seg_next, q_prev, k_prev, v_prev, seg_prev, upstream, flags,
    attn_v, gq_v, gk_v, gv_v,
    own, near, far, side, side_grads, side_recv, grads, far_send, far_recv, near_send, near_recv,
    q_prev_v, up_v, q_next_v, flags_v, seg_prev_v, seg_next_v, dq_t, bias, count_send, count_recv,
    load_sem, array_sem, send_sem, recv_sem, gsend_sem, grecv_sem, csend_sem, crecv_sem,
):
    kv_heads, n_fsdp, n_seq, plan = sizes
    chunks = 2 * kv_heads
    width = GROUP * HEAD_DIM
    seq_at = lax.axis_index("seq")
    fsdp_at = lax.axis_index("fsdp")
    core = seq_at % 2
    ahead_at = (seq_at + 2) % n_seq
    behind_at = (seq_at + n_seq - 2) % n_seq
    side_at = seq_at + 1 - 2 * core
    scale = HEAD_DIM ** -0.5

    partners = [
        [
            {axis: at + ((at // stride % radix + j) % radix - at // stride % radix) * stride}
            for j in range(1, radix)
        ]
        for axis, stride, radix in plan
        for at in ((seq_at if axis == "seq" else fsdp_at),)
    ]
    rounds = len(plan)

    def remote(src, dst, sems, at, device):
        return pltpu.make_async_remote_copy(
            src_ref=src, dst_ref=dst, send_sem=sems[0].at[at], recv_sem=sems[1].at[at],
            device_id=device, device_id_type=MESH,
        )

    links = (send_sem, recv_sem)
    glinks = (gsend_sem, grecv_sem)

    def own_ahead(t):
        return remote(own.at[t], near.at[t], links, (0, t), {"seq": ahead_at})

    def near_ahead(t):
        return remote(near.at[t], far.at[t], links, (1, t), {"seq": ahead_at})

    def own_side(t):
        return remote(own.at[t], side.at[0, t], links, (2, t), {"seq": side_at})

    def near_side(t):
        return remote(near.at[t], side.at[1, t], links, (3, t), {"seq": side_at})

    def far_side(t):
        return remote(far.at[t], side.at[2, t], links, (4, t), {"seq": side_at})

    def grads_side(t):
        return remote(side_grads.at[t], side_recv.at[t], glinks, (0, t), {"seq": side_at})

    def far_back(t):
        return remote(far_send.at[t], far_recv.at[t], glinks, (1, t), {"seq": behind_at})

    def near_back(t):
        return remote(near_send.at[t], near_recv.at[t], glinks, (2, t), {"seq": behind_at})

    def counts_to(r):
        return [
            remote(
                count_send.at[r], count_recv.at[r, j], (csend_sem, crecv_sem), (r, j), partner
            )
            for j, partner in enumerate(partners[r])
        ]

    def load(t, which):
        k_from, v_from = (k_prev, v_prev) if t < kv_heads else (k_next, v_next)
        src = (k_from, v_from)[which]
        columns = slice((t % kv_heads) * HEAD_DIM, (t % kv_heads + 1) * HEAD_DIM)
        return pltpu.make_async_copy(src.at[:, columns], own.at[t, which], load_sem.at[t, which])

    def wait_load(t):
        for which, src in enumerate((k_prev, v_prev)):
            pltpu.make_async_copy(
                src.at[:, 0:HEAD_DIM], own.at[t, which], load_sem.at[t, which]
            ).wait()

    def columns_of(g, count=GROUP):
        return pl.ds(pl.multiple_of(g * (count * HEAD_DIM), HEAD_DIM), count * HEAD_DIM)

    barrier = pltpu.get_barrier_semaphore()
    peers = [{"seq": ahead_at}, {"seq": behind_at}] + sum(partners, [])
    for peer in peers:
        pl.semaphore_signal(barrier, inc=1, device_id=peer, device_id_type=MESH)

    small = ((flags, flags_v), (seg_prev, seg_prev_v), (seg_next, seg_next_v))
    small_copies = [
        pltpu.make_async_copy(src, dst, array_sem.at[3 + i]) for i, (src, dst) in enumerate(small)
    ]
    for copy in small_copies:
        copy.start()
    for t in range(chunks):
        load(t, 0).start()
        load(t, 1).start()
    arrays = ((q_prev, q_prev_v), (upstream, up_v), (q_next, q_next_v))
    array_copies = [
        pltpu.make_async_copy(src, dst, array_sem.at[i]) for i, (src, dst) in enumerate(arrays)
    ]
    for copy in array_copies:
        copy.start()

    for copy in small_copies:
        copy.wait()
    count_send[0] = jnp.broadcast_to(
        jnp.sum(flags_v[...].astype(F32), axis=1, keepdims=True), count_send.shape[1:]
    )

    rows_at = lax.broadcasted_iota(jnp.int32, (HEAD_DIM, HEAD_DIM), 0)
    lanes_at = lax.broadcasted_iota(jnp.int32, (HEAD_DIM, HEAD_DIM), 1)
    for m, seg in enumerate((seg_prev_v, seg_next_v)):
        def ids_at(index, seg=seg):
            return seg[:, pl.ds(pl.multiple_of(index * HEAD_DIM, HEAD_DIM), HEAD_DIM)].astype(F32)

        q_ids = ids_at(seq_at)
        for d in range(BLOCKS):
            k_ids = column_of(ids_at((seq_at + n_seq - d) % n_seq))
            keep = k_ids == q_ids
            if d == 0:
                keep = keep & (rows_at <= lanes_at)
                block_bias = jnp.where(keep, 0.0, -1e30)
            else:
                block_bias = jnp.where(keep, 0.0, -1e30)
                block_bias = jnp.where(seq_at >= d, block_bias, -1e30)
            bias[m, d * HEAD_DIM : (d + 1) * HEAD_DIM, :] = block_bias

    for t in range(AHEAD):
        wait_load(t)
    pl.semaphore_wait(barrier, len(peers))
    for copy in counts_to(0):
        copy.start()
    for t in range(AHEAD):
        own_ahead(t).start()
        own_side(t).start()

    def window(w, which):
        return jnp.concatenate(
            [own[w, which], side[1 - core, w, which], near[w, which],
             side[2 - core, w, which], far[w, which]],
            axis=0,
        )

    def stacked(ref, g, first, count):
        return jnp.concatenate(
            [
                ref[:, pl.ds(pl.multiple_of(g * width + j * HEAD_DIM, HEAD_DIM), HEAD_DIM)]
                for j in range(first, first + count)
            ],
            axis=0,
        )

    def expo(k_all, q_part, m):
        pair = bias[m]
        scores = dot(k_all, q_part, ((1,), (1,))) + jnp.concatenate([pair, pair], axis=1)
        top = jnp.max(scores, axis=0, keepdims=True)
        values = jnp.exp2((scores - top) * (scale * math.log2(math.e)))
        return values, 1.0 / jnp.sum(values, axis=0, keepdims=True)

    def backward(w):
        k_all, v_all = window(w, 0), window(w, 1)
        k_turned = jnp.transpose(k_all)
        flag_row = flags_v[...].astype(F32)
        flag_pair = jnp.concatenate([flag_row, flag_row], axis=1)
        dk = dv = None
        for half in range(2):
            q_part = stacked(q_prev_v, w, 2 * half, 2)
            u_part = stacked(up_v, w, 2 * half, 2)
            values, inverse = expo(k_all, q_part, 0)
            d_probs = dot(v_all, u_part, ((1,), (1,)))
            row_delta = jnp.sum(values * d_probs, axis=0, keepdims=True) * inverse
            probs = values * (inverse * flag_pair)
            d_scores = (probs * (d_probs - row_delta)).astype(BF16)
            dq_t[w, :, half * 256 : (half + 1) * 256] = dot(k_turned, d_scores, ((1,), (0,)))
            dk_part = dot(d_scores, q_part, ((1,), (0,)))
            dv_part = dot(probs.astype(BF16), u_part, ((1,), (0,)))
            dk = dk_part if dk is None else dk + dk_part
            dv = dv_part if dv is None else dv + dv_part
        for which, total in enumerate((dk, dv)):
            for d in range(BLOCKS):
                block = total[d * HEAD_DIM : (d + 1) * HEAD_DIM]
                if d % 2:
                    side_grads[w, d // 2, which] = block.astype(BF16)
                else:
                    grads[w, d // 2, which] = block

    def forward(w):
        g = w - kv_heads
        k_all, v_turned = window(w, 0), jnp.transpose(window(w, 1))
        for half in range(2):
            values, inverse = expo(k_all, stacked(q_next_v, g, 2 * half, 2), 1)
            mixed = dot(v_turned, values.astype(BF16), ((1,), (0,))) * inverse
            for j in range(2):
                at = pl.multiple_of(g * width + (2 * half + j) * HEAD_DIM, HEAD_DIM)
                attn_v[:, pl.ds(at, HEAD_DIM)] = jnp.transpose(
                    mixed[:, j * HEAD_DIM : (j + 1) * HEAD_DIM]
                ).astype(BF16)

    def factor_row():
        total = count_send[rounds, 0:1, :]
        return (HEAD_DIM * n_fsdp * n_seq) / jnp.maximum(total, 1.0)

    def finish_q(g):
        gain = factor_row() * scale
        for j in range(GROUP):
            at = pl.multiple_of(g * width + j * HEAD_DIM, HEAD_DIM)
            turned = jnp.transpose(dq_t[g, :, j * HEAD_DIM : (j + 1) * HEAD_DIM])
            gq_v[:, pl.ds(at, HEAD_DIM)] = (turned * gain).astype(BF16)

    def take_side(w):
        for part in range(2):
            grads[w, core + part] = grads[w, core + part] + side_recv[w, part].astype(F32)
        far_send[w] = grads[w, 2].astype(BF16)

    def take_far(w):
        near_send[w] = (grads[w, 1] + far_recv[w].astype(F32)).astype(BF16)

    def take_near(w):
        total = grads[w, 0] + near_recv[w].astype(F32)
        gain = factor_row()
        gk_v[:, columns_of(w, 1)] = (total[0] * (gain * scale)).astype(BF16)
        gv_v[:, columns_of(w, 1)] = (total[1] * gain).astype(BF16)

    def during(t, first, count):
        return pl.when((t >= first) & (t < first + count))

    for copy in array_copies:
        copy.wait()

    late = max(LAG + kv_heads // 2 + 7, COUNT_STEPS * rounds)

    def one_step(t, carry):
        @during(t, 0, chunks - AHEAD)
        def _():
            wait_load(t + AHEAD)
            own_ahead(t + AHEAD).start()
            own_side(t + AHEAD).start()

        @during(t, 0, chunks)
        def _():
            own_ahead(t).wait_recv()
            near_ahead(t).start()
            near_side(t).start()

        @during(t, LAG - 1, chunks)
        def _():
            near_ahead(t - LAG + 1).wait_recv()
            far_side(t - LAG + 1).start()

        @during(t, LAG + 1, kv_heads)
        def _():
            grads_side(t - LAG - 1).start()

        @during(t, LAG + 2, kv_heads)
        def _():
            grads_side(t - LAG - 2).wait_recv()
            take_side(t - LAG - 2)

        @during(t, LAG + 5, kv_heads)
        def _():
            far_back(t - LAG - 5).wait_recv()
            take_far(t - LAG - 5)

        for r in range(rounds):
            @pl.when(t == COUNT_STEPS * (r + 1) - 1)
            def _(r=r):
                total = count_send[r]
                for j, copy in enumerate(counts_to(r)):
                    copy.wait_recv()
                    total = total + count_recv[r, j]
                count_send[r + 1] = total

        @during(t, late, kv_heads // 2)
        def _():
            for which in range(2):
                w = 2 * (t - late) + which
                near_back(w).wait_recv()
                take_near(w)

        @during(t, LAG, chunks)
        def _():
            w = t - LAG
            own_side(w).wait_recv()
            near_side(w).wait_recv()
            far_side(w).wait_recv()

        @during(t, LAG, kv_heads)
        def _():
            backward(t - LAG)

        @during(t, LAG + kv_heads, kv_heads)
        def _():
            forward(t - LAG)

        @during(t, late - 1, kv_heads // 2)
        def _():
            for which in range(2):
                finish_q(2 * (t - late + 1) + which)

        @during(t, LAG + 2, kv_heads)
        def _():
            far_back(t - LAG - 2).start()

        @during(t, LAG + 5, kv_heads)
        def _():
            near_back(t - LAG - 5).start()

        for r in range(1, rounds):
            @pl.when(t == COUNT_STEPS * r - 1)
            def _(r=r):
                for copy in counts_to(r):
                    copy.start()

        return carry

    steps = max(chunks + LAG, late + kv_heads // 2, COUNT_STEPS * rounds + 1)
    lax.fori_loop(0, steps, one_step, 0)

    def drain(t, carry):
        own_ahead(t).wait_send()
        near_ahead(t).wait_send()
        own_side(t).wait_send()
        near_side(t).wait_send()
        far_side(t).wait_send()
        return carry

    lax.fori_loop(0, chunks, drain, 0)

    def drain_back(g, carry):
        grads_side(g).wait_send()
        far_back(g).wait_send()
        near_back(g).wait_send()
        return carry

    lax.fori_loop(0, kv_heads, drain_back, 0)
    for r in range(rounds):
        for copy in counts_to(r):
            copy.wait_send()


def write_out(*refs):
    ins, outs, sems = refs[:4], refs[4:8], refs[8]
    copies = [pltpu.make_async_copy(ins[i], outs[i], sems.at[i]) for i in range(4)]
    for copy in copies:
        copy.start()
    for copy in copies:
        copy.wait()


def count_plan(n_fsdp, n_seq):
    plan = []
    for axis, size in (("seq", n_seq), ("fsdp", n_fsdp)):
        stride = 1
        while stride < size:
            radix = min(8, size // stride)
            plan.append((axis, stride, radix))
            stride *= radix
    first = plan.pop(0)
    return [first] + plan[::-1]


def body(n_fsdp, n_seq, *args):
    q, k = args[0], args[1]
    rows = q.shape[0]
    kv_heads = k.shape[1] // HEAD_DIM
    chunks = 2 * kv_heads
    width = q.shape[1]
    plan = count_plan(n_fsdp, n_seq)
    rounds, most = len(plan), max(radix for _, _, radix in plan) - 1
    tile = (2, HEAD_DIM, HEAD_DIM)
    anywhere = pl.BlockSpec(memory_space=pl.ANY)
    vmem = pl.BlockSpec(memory_space=pltpu.VMEM)
    dma = pltpu.SemaphoreType.DMA
    done = pl.pallas_call(
        functools.partial(kernel, (kv_heads, n_fsdp, n_seq, plan)),
        out_shape=tuple(pltpu.VMEM(x.shape, BF16) for x in (q, q, k, k)),
        in_specs=[pl.BlockSpec(memory_space=pltpu.HBM)] * 10,
        out_specs=(vmem,) * 4,
        scratch_shapes=[
            pltpu.VMEM((chunks,) + tile, BF16),
            pltpu.VMEM((chunks,) + tile, BF16),
            pltpu.VMEM((chunks,) + tile, BF16),
            pltpu.VMEM((3, chunks) + tile, BF16),
            pltpu.VMEM((kv_heads, 2) + tile, BF16),
            pltpu.VMEM((kv_heads, 2) + tile, BF16),
            pltpu.VMEM((kv_heads, 3) + tile, F32),
            pltpu.VMEM((kv_heads,) + tile, BF16),
            pltpu.VMEM((kv_heads,) + tile, BF16),
            pltpu.VMEM((kv_heads,) + tile, BF16),
            pltpu.VMEM((kv_heads,) + tile, BF16),
            pltpu.VMEM((rows, width), BF16),
            pltpu.VMEM((rows, width), BF16),
            pltpu.VMEM((rows, width), BF16),
            pltpu.VMEM(args[9].shape, jnp.int32),
            pltpu.VMEM(args[7].shape, jnp.int32),
            pltpu.VMEM(args[3].shape, jnp.int32),
            pltpu.VMEM((kv_heads, HEAD_DIM, GROUP * HEAD_DIM), F32),
            pltpu.VMEM((2, BLOCKS * HEAD_DIM, HEAD_DIM), F32),
            pltpu.VMEM((rounds + 1, 8, 128), F32),
            pltpu.VMEM((rounds, most, 8, 128), F32),
            dma((chunks, 2)),
            dma((6,)),
            dma((5, chunks)),
            dma((5, chunks)),
            dma((3, kv_heads)),
            dma((3, kv_heads)),
            dma((rounds, most)),
            dma((rounds, most)),
        ],
        compiler_params=pltpu.CompilerParams(
            collective_id=0, has_side_effects=True, vmem_limit_bytes=60 * 1024 * 1024
        ),
    )(*args)
    return pl.pallas_call(
        write_out,
        out_shape=tuple(jax.ShapeDtypeStruct(x.shape, BF16) for x in (q, q, k, k)),
        in_specs=[anywhere] * 4,
        out_specs=(anywhere,) * 4,
        scratch_shapes=[dma((4,))],
        compiler_params=pltpu.CompilerParams(vmem_limit_bytes=8 * 1024 * 1024),
    )(*(pltpu.with_memory_space_constraint(x, pltpu.VMEM) for x in done))


def solution(mesh):
    both = P(("fsdp", "seq"), None)
    ids = P("fsdp", None)
    return jax.shard_map(
        functools.partial(body, mesh.shape["fsdp"], mesh.shape["seq"]),
        mesh=mesh,
        in_specs=(both, both, both, ids, both, both, both, ids, both, P("fsdp", "seq")),
        out_specs=(both,) * 4,
        check_vma=False,
    )
```

```python
import functools
import math

import jax
import jax.numpy as jnp
from jax import lax
from jax.experimental import pallas as pl
from jax.experimental.pallas import tpu as pltpu
from jax.sharding import PartitionSpec as P

HEAD_DIM = 128
GROUP = 4
BLOCKS = 5
AHEAD = 2
COUNT_STEPS = 4
TURNS = 8
LAG = 4
MESH = pl.DeviceIdType.MESH
F32 = jnp.float32
BF16 = jnp.bfloat16


def dot(a, b, dims):
    return lax.dot_general(a, b, (dims, ((), ())), preferred_element_type=F32)


def over_keys(values, join, reduce):
    blocks = [values[d * HEAD_DIM : (d + 1) * HEAD_DIM] for d in range(BLOCKS)]
    return reduce(functools.reduce(join, blocks), axis=0, keepdims=True)


def column_of(row):
    return jnp.transpose(jnp.broadcast_to(row, (128, row.shape[1])))


def kernel(
    sizes,
    q_next, k_next, v_next, seg_next, q_prev, k_prev, v_prev, seg_prev, upstream, flags,
    attn_v, gq_v, gk_v, gv_v,
    held, side, side_grads, side_recv, grads, far_send, far_recv, near_send, near_recv,
    arrays_v, flags_v, seg_prev_v, seg_next_v, dq_t, bias, count_send, count_recv,
    load_sem, small_sem, send_sem, recv_sem, gsend_sem, grecv_sem, csend_sem, crecv_sem,
):
    kv_heads, n_fsdp, n_seq, plan = sizes
    chunks = 2 * kv_heads
    width = GROUP * HEAD_DIM
    seq_at = lax.axis_index("seq")
    fsdp_at = lax.axis_index("fsdp")
    core = seq_at % 2
    ahead_at = (seq_at + 2) % n_seq
    behind_at = (seq_at + n_seq - 2) % n_seq
    side_at = seq_at + 1 - 2 * core
    scale = HEAD_DIM ** -0.5

    partners = [
        [
            {axis: at + ((at // stride % radix + j) % radix - at // stride % radix) * stride}
            for j in range(1, radix)
        ]
        for axis, stride, radix in plan
        for at in ((seq_at if axis == "seq" else fsdp_at),)
    ]
    rounds = len(plan)

    def remote(src, dst, sent, received, device):
        return pltpu.make_async_remote_copy(
            src_ref=src, dst_ref=dst, send_sem=sent, recv_sem=received,
            device_id=device, device_id_type=MESH,
        )

    def pass_on(t, kind, src, dst, device):
        return remote(
            src, dst, send_sem.at[kind, t % TURNS], recv_sem.at[kind, t], {"seq": device}
        )

    def own_ahead(t):
        return pass_on(t, 0, held.at[t, 0], held.at[t, 1], ahead_at)

    def near_ahead(t):
        return pass_on(t, 1, held.at[t, 1], held.at[t, 2], ahead_at)

    def all_side(t):
        return pass_on(t, 2, held.at[t], side.at[t], side_at)

    def give_back(t, kind, src, dst, device):
        return remote(
            src, dst, gsend_sem.at[kind, t % TURNS], grecv_sem.at[kind, t], {"seq": device}
        )

    def grads_side(t):
        return give_back(t, 0, side_grads.at[t], side_recv.at[t], side_at)

    def far_back(t):
        return give_back(t, 1, far_send.at[t], far_recv.at[t], behind_at)

    def near_back(t):
        return give_back(t, 2, near_send.at[t], near_recv.at[t], behind_at)

    def counts_to(r):
        return [
            remote(
                count_send.at[r], count_recv.at[r, j], csend_sem.at[j], crecv_sem.at[r, j], partner
            )
            for j, partner in enumerate(partners[r])
        ]

    def load(t, which):
        k_from, v_from = (k_prev, v_prev) if t < kv_heads else (k_next, v_next)
        src = (k_from, v_from)[which]
        columns = slice((t % kv_heads) * HEAD_DIM, (t % kv_heads + 1) * HEAD_DIM)
        return pltpu.make_async_copy(
            src.at[:, columns], held.at[t, 0, which], load_sem.at[int(t >= AHEAD)]
        )

    def wait_loads(first, last):
        part = held.at[first:last, 0]
        pltpu.make_async_copy(part, part, load_sem.at[int(first >= AHEAD)]).wait()

    def columns_of(g, count=GROUP):
        return pl.ds(pl.multiple_of(g * (count * HEAD_DIM), HEAD_DIM), count * HEAD_DIM)

    barrier = pltpu.get_barrier_semaphore()
    peers = [{"seq": ahead_at}, {"seq": behind_at}] + sum(partners, [])
    for peer in peers:
        pl.semaphore_signal(barrier, inc=1, device_id=peer, device_id_type=MESH)

    for t in range(AHEAD):
        load(t, 0).start()
        load(t, 1).start()
    small = ((flags, flags_v), (seg_prev, seg_prev_v), (seg_next, seg_next_v))
    small_copies = [
        pltpu.make_async_copy(src, dst, small_sem.at[i]) for i, (src, dst) in enumerate(small)
    ]
    for copy in small_copies:
        copy.start()
    for t in range(AHEAD, chunks):
        load(t, 0).start()
        load(t, 1).start()
    for i, src in enumerate((q_prev, upstream, q_next)):
        pltpu.make_async_copy(src, arrays_v.at[i], load_sem.at[2]).start()

    wait_loads(0, AHEAD)
    pl.semaphore_wait(barrier, len(peers))
    for t in range(AHEAD):
        own_ahead(t).start()

    for copy in small_copies:
        copy.wait()
    count_send[0] = jnp.broadcast_to(
        jnp.sum(flags_v[...].astype(F32), axis=1, keepdims=True), count_send.shape[1:]
    )

    rows_at = lax.broadcasted_iota(jnp.int32, (HEAD_DIM, HEAD_DIM), 0)
    lanes_at = lax.broadcasted_iota(jnp.int32, (HEAD_DIM, HEAD_DIM), 1)
    for m, seg in enumerate((seg_prev_v, seg_next_v)):
        def ids_at(index, seg=seg):
            return seg[:, pl.ds(pl.multiple_of(index * HEAD_DIM, HEAD_DIM), HEAD_DIM)].astype(F32)

        q_ids = ids_at(seq_at)
        for d in range(BLOCKS):
            k_ids = column_of(ids_at((seq_at + n_seq - d) % n_seq))
            keep = k_ids == q_ids
            if d == 0:
                keep = keep & (rows_at <= lanes_at)
                block_bias = jnp.where(keep, 0.0, -1e30)
            else:
                block_bias = jnp.where(keep, 0.0, -1e30)
                block_bias = jnp.where(seq_at >= d, block_bias, -1e30)
            bias[m, d * HEAD_DIM : (d + 1) * HEAD_DIM, :] = block_bias

    for copy in counts_to(0):
        copy.start()
    wait_loads(AHEAD, chunks)
    pltpu.make_async_copy(arrays_v, arrays_v, load_sem.at[2]).wait()

    def window(w, which):
        return jnp.concatenate(
            [held[w, 0, which], side[w, 1 - core, which], held[w, 1, which],
             side[w, 2 - core, which], held[w, 2, which]],
            axis=0,
        )

    def stacked(i, g, first, count):
        return jnp.concatenate(
            [
                arrays_v[i, :, pl.ds(pl.multiple_of(g * width + j * HEAD_DIM, HEAD_DIM), HEAD_DIM)]
                for j in range(first, first + count)
            ],
            axis=0,
        )

    def expo(k_all, q_part, m):
        pair = bias[m]
        scores = dot(k_all, q_part, ((1,), (1,))) + jnp.concatenate([pair, pair], axis=1)
        top = over_keys(scores, jnp.maximum, jnp.max)
        values = jnp.exp2((scores - top) * (scale * math.log2(math.e)))
        return values, 1.0 / over_keys(values, jnp.add, jnp.sum)

    def backward(w):
        k_all, v_all = window(w, 0), window(w, 1)
        k_turned = jnp.transpose(k_all)
        flag_row = flags_v[...].astype(F32)
        flag_pair = jnp.concatenate([flag_row, flag_row], axis=1)
        dk = dv = None
        for half in range(2):
            q_part = stacked(0, w, 2 * half, 2)
            u_part = stacked(1, w, 2 * half, 2)
            values, inverse = expo(k_all, q_part, 0)
            d_probs = dot(v_all, u_part, ((1,), (1,)))
            row_delta = over_keys(values * d_probs, jnp.add, jnp.sum) * inverse
            probs = values * (inverse * flag_pair)
            d_scores = (probs * (d_probs - row_delta)).astype(BF16)
            dq_t[w, :, half * 256 : (half + 1) * 256] = dot(k_turned, d_scores, ((1,), (0,)))
            dk_part = dot(d_scores, q_part, ((1,), (0,)))
            dv_part = dot(probs.astype(BF16), u_part, ((1,), (0,)))
            dk = dk_part if dk is None else dk + dk_part
            dv = dv_part if dv is None else dv + dv_part
        for which, total in enumerate((dk, dv)):
            for d in range(BLOCKS):
                block = total[d * HEAD_DIM : (d + 1) * HEAD_DIM]
                if d % 2:
                    side_grads[w, d // 2, which] = block.astype(BF16)
                else:
                    grads[w, d // 2, which] = block

    def forward(w):
        g = w - kv_heads
        k_all, v_all = window(w, 0), window(w, 1)
        lower = jnp.concatenate([rows_at <= lanes_at] * GROUP, axis=1)
        scores = dot(k_all, stacked(2, g, 0, GROUP), ((1,), (1,)))
        scores = scores + jnp.concatenate([bias[1]] * GROUP, axis=1)
        blocks = [scores[d * HEAD_DIM : (d + 1) * HEAD_DIM] for d in range(BLOCKS)]
        blocks = [jnp.where(lower, blocks[0], blocks[4])] + blocks[1:4]
        top = jnp.max(functools.reduce(jnp.maximum, blocks), axis=0, keepdims=True)
        values = [jnp.exp2((x - top) * (scale * math.log2(math.e))) for x in blocks]
        inverse = 1.0 / jnp.sum(functools.reduce(jnp.add, values), axis=0, keepdims=True)
        ends = jnp.where(lower, values[0], 0.0), jnp.where(lower, 0.0, values[0])
        parts = [x.astype(BF16) for x in [ends[0]] + values[1:] + [ends[1]]]
        mixed = dot(jnp.transpose(v_all), jnp.concatenate(parts, axis=0), ((1,), (0,))) * inverse
        for j in range(GROUP):
            at = pl.multiple_of(g * width + j * HEAD_DIM, HEAD_DIM)
            attn_v[:, pl.ds(at, HEAD_DIM)] = jnp.transpose(
                mixed[:, j * HEAD_DIM : (j + 1) * HEAD_DIM]
            ).astype(BF16)

    def factor_row():
        total = count_send[rounds, 0:1, :]
        return (HEAD_DIM * n_fsdp * n_seq) / jnp.maximum(total, 1.0)

    def finish_q(g):
        gain = factor_row() * scale
        for j in range(GROUP):
            at = pl.multiple_of(g * width + j * HEAD_DIM, HEAD_DIM)
            turned = jnp.transpose(dq_t[g, :, j * HEAD_DIM : (j + 1) * HEAD_DIM])
            gq_v[:, pl.ds(at, HEAD_DIM)] = (turned * gain).astype(BF16)

    def take_side(w):
        for part in range(2):
            grads[w, core + part] = grads[w, core + part] + side_recv[w, part].astype(F32)
        far_send[w] = grads[w, 2].astype(BF16)

    def take_far(w):
        near_send[w] = (grads[w, 1] + far_recv[w].astype(F32)).astype(BF16)

    def take_near(w):
        total = grads[w, 0] + near_recv[w].astype(F32)
        gain = factor_row()
        gk_v[:, columns_of(w, 1)] = (total[0] * (gain * scale)).astype(BF16)
        gv_v[:, columns_of(w, 1)] = (total[1] * gain).astype(BF16)

    def during(t, first, count):
        return pl.when((t >= first) & (t < first + count))

    late = max(LAG + kv_heads // 2 + 8, COUNT_STEPS * rounds + 3)

    def one_step(t, carry):
        @during(t, 0, chunks - AHEAD)
        def _():
            own_ahead(t + AHEAD).start()

        @during(t, 0, chunks)
        def _():
            own_ahead(t).wait_recv()
            near_ahead(t).start()

        @during(t, LAG - 1, chunks)
        def _():
            near_ahead(t - LAG + 1).wait_recv()
            all_side(t - LAG + 1).start()

        @during(t, LAG + 1, kv_heads)
        def _():
            grads_side(t - LAG - 1).start()

        @during(t, LAG + 2, kv_heads)
        def _():
            grads_side(t - LAG - 2).wait_recv()
            take_side(t - LAG - 2)

        @during(t, LAG + 5, kv_heads)
        def _():
            far_back(t - LAG - 5).wait_recv()
            take_far(t - LAG - 5)

        for r in range(rounds):
            @pl.when(t == COUNT_STEPS * (r + 1) - 1)
            def _(r=r):
                total = count_send[r]
                for j, copy in enumerate(counts_to(r)):
                    copy.wait()
                    total = total + count_recv[r, j]
                count_send[r + 1] = total

        @during(t, LAG, chunks)
        def _():
            all_side(t - LAG).wait_recv()

        @during(t, LAG, kv_heads)
        def _():
            backward(t - LAG)

        @during(t, LAG + kv_heads, kv_heads)
        def _():
            forward(t - LAG)

        @during(t, late - 4, kv_heads // 2)
        def _():
            for which in range(2):
                finish_q(2 * (t - late + 4) + which)

        @during(t, LAG + 2, kv_heads)
        def _():
            far_back(t - LAG - 2).start()

        @during(t, LAG + 5, kv_heads)
        def _():
            near_back(t - LAG - 5).start()

        for r in range(1, rounds):
            @pl.when(t == COUNT_STEPS * r - 1)
            def _(r=r):
                for copy in counts_to(r):
                    copy.start()

        @during(t, late, kv_heads // 2)
        def _():
            for which in range(2):
                w = 2 * (t - late) + which
                near_back(w).wait_recv()
                take_near(w)

        @during(t, LAG, chunks)
        def _():
            own_ahead(t - LAG).wait_send()
            near_ahead(t - LAG).wait_send()
            all_side(t - LAG).wait_send()

        @during(t, LAG + 8, kv_heads)
        def _():
            grads_side(t - LAG - 8).wait_send()
            far_back(t - LAG - 8).wait_send()
            near_back(t - LAG - 8).wait_send()

        return carry

    steps = max(chunks + LAG, late + kv_heads // 2, kv_heads + LAG + 8, COUNT_STEPS * rounds + 1)
    lax.fori_loop(0, steps, one_step, 0)


def write_out(*refs):
    ins, outs, sems = refs[:4], refs[4:8], refs[8]
    copies = [pltpu.make_async_copy(ins[i], outs[i], sems.at[i]) for i in range(4)]
    for copy in copies:
        copy.start()
    for copy in copies:
        copy.wait()


def count_plan(n_fsdp, n_seq):
    plan = []
    for axis, size in (("seq", n_seq), ("fsdp", n_fsdp)):
        stride = 1
        while stride < size:
            radix = min(8, size // stride)
            plan.append((axis, stride, radix))
            stride *= radix
    first = plan.pop(0)
    return [first] + plan[::-1]


def body(n_fsdp, n_seq, *args):
    q, k = args[0], args[1]
    rows = q.shape[0]
    kv_heads = k.shape[1] // HEAD_DIM
    chunks = 2 * kv_heads
    width = q.shape[1]
    plan = count_plan(n_fsdp, n_seq)
    rounds, most = len(plan), max(radix for _, _, radix in plan) - 1
    tile = (2, HEAD_DIM, HEAD_DIM)
    anywhere = pl.BlockSpec(memory_space=pl.ANY)
    vmem = pl.BlockSpec(memory_space=pltpu.VMEM)
    dma = pltpu.SemaphoreType.DMA
    done = pl.pallas_call(
        functools.partial(kernel, (kv_heads, n_fsdp, n_seq, plan)),
        out_shape=tuple(pltpu.VMEM(x.shape, BF16) for x in (q, q, k, k)),
        in_specs=[pl.BlockSpec(memory_space=pltpu.HBM)] * 10,
        out_specs=(vmem,) * 4,
        scratch_shapes=[
            pltpu.VMEM((chunks, 3) + tile, BF16),
            pltpu.VMEM((chunks, 3) + tile, BF16),
            pltpu.VMEM((kv_heads, 2) + tile, BF16),
            pltpu.VMEM((kv_heads, 2) + tile, BF16),
            pltpu.VMEM((kv_heads, 3) + tile, F32),
            pltpu.VMEM((kv_heads,) + tile, BF16),
            pltpu.VMEM((kv_heads,) + tile, BF16),
            pltpu.VMEM((kv_heads,) + tile, BF16),
            pltpu.VMEM((kv_heads,) + tile, BF16),
            pltpu.VMEM((3, rows, width), BF16),
            pltpu.VMEM(args[9].shape, jnp.int32),
            pltpu.VMEM(args[7].shape, jnp.int32),
            pltpu.VMEM(args[3].shape, jnp.int32),
            pltpu.VMEM((kv_heads, HEAD_DIM, GROUP * HEAD_DIM), F32),
            pltpu.VMEM((2, BLOCKS * HEAD_DIM, HEAD_DIM), F32),
            pltpu.VMEM((rounds + 1, 8, 128), F32),
            pltpu.VMEM((rounds, most, 8, 128), F32),
            dma((3,)),
            dma((3,)),
            dma((3, TURNS)),
            dma((3, chunks)),
            dma((3, TURNS)),
            dma((3, kv_heads)),
            dma((most,)),
            dma((rounds, most)),
        ],
        compiler_params=pltpu.CompilerParams(
            collective_id=0, has_side_effects=True, vmem_limit_bytes=60 * 1024 * 1024
        ),
    )(*args)
    return pl.pallas_call(
        write_out,
        out_shape=tuple(jax.ShapeDtypeStruct(x.shape, BF16) for x in (q, q, k, k)),
        in_specs=[anywhere] * 4,
        out_specs=(anywhere,) * 4,
        scratch_shapes=[dma((4,))],
        compiler_params=pltpu.CompilerParams(vmem_limit_bytes=8 * 1024 * 1024),
    )(*(pltpu.with_memory_space_constraint(x, pltpu.VMEM) for x in done))


def solution(mesh):
    both = P(("fsdp", "seq"), None)
    ids = P("fsdp", None)
    return jax.shard_map(
        functools.partial(body, mesh.shape["fsdp"], mesh.shape["seq"]),
        mesh=mesh,
        in_specs=(both, both, both, ids, both, both, both, ids, both, P("fsdp", "seq")),
        out_specs=(both,) * 4,
        check_vma=False,
    )
```

```python
import functools
import math

import jax
import jax.numpy as jnp
from jax import lax
from jax.experimental import pallas as pl
from jax.experimental.pallas import tpu as pltpu
from jax.sharding import PartitionSpec as P

HEAD_DIM = 128
GROUP = 4
BLOCKS = 5
AHEAD = 2
COUNT_STEPS = 4
TURNS = 8
LAG = 4
MESH = pl.DeviceIdType.MESH
F32 = jnp.float32
BF16 = jnp.bfloat16


def dot(a, b, dims):
    return lax.dot_general(a, b, (dims, ((), ())), preferred_element_type=F32)


def over_keys(values, join, reduce):
    blocks = [values[d * HEAD_DIM : (d + 1) * HEAD_DIM] for d in range(BLOCKS)]
    return reduce(functools.reduce(join, blocks), axis=0, keepdims=True)


def column_of(row):
    return jnp.transpose(jnp.broadcast_to(row, (128, row.shape[1])))


def kernel(
    sizes,
    q_next, k_next, v_next, seg_next, q_prev, k_prev, v_prev, seg_prev, upstream, flags,
    attn_v, gq_v, gk_v, gv_v,
    held, side, side_grads, side_recv, grads, far_send, far_recv, near_send, near_recv,
    arrays_v, flags_v, seg_prev_v, seg_next_v, dq_t, bias, count_send, count_recv,
    load_sem, small_sem, send_sem, recv_sem, gsend_sem, grecv_sem, csend_sem, crecv_sem,
):
    kv_heads, n_fsdp, n_seq, plan = sizes
    chunks = 2 * kv_heads
    width = GROUP * HEAD_DIM
    seq_at = lax.axis_index("seq")
    fsdp_at = lax.axis_index("fsdp")
    core = seq_at % 2
    ahead_at = (seq_at + 2) % n_seq
    behind_at = (seq_at + n_seq - 2) % n_seq
    side_at = seq_at + 1 - 2 * core
    chip_at, last_chip = seq_at // 2, n_seq // 2 - 1
    has_next, has_behind = chip_at < last_chip, chip_at > 0
    scale = HEAD_DIM ** -0.5

    partners = [
        [
            {axis: at + ((at // stride % radix + j) % radix - at // stride % radix) * stride}
            for j in range(1, radix)
        ]
        for axis, stride, radix in plan
        for at in ((seq_at if axis == "seq" else fsdp_at),)
    ]
    rounds = len(plan)

    def remote(src, dst, sent, received, device):
        return pltpu.make_async_remote_copy(
            src_ref=src, dst_ref=dst, send_sem=sent, recv_sem=received,
            device_id=device, device_id_type=MESH,
        )

    def pass_on(t, kind, src, dst, device):
        return remote(
            src, dst, send_sem.at[kind, t % TURNS], recv_sem.at[kind, t], {"seq": device}
        )

    def own_ahead(t):
        return pass_on(t, 0, held.at[t, 0], held.at[t, 1], ahead_at)

    def near_ahead(t):
        return pass_on(t, 1, held.at[t, 1], held.at[t, 2], ahead_at)

    def all_side(t):
        return pass_on(t, 2, held.at[t], side.at[t], side_at)

    def give_back(t, kind, src, dst, device):
        return remote(
            src, dst, gsend_sem.at[kind, t % TURNS], grecv_sem.at[kind, t], {"seq": device}
        )

    def grads_side(t):
        return give_back(t, 0, side_grads.at[t], side_recv.at[t], side_at)

    def far_back(t):
        return give_back(t, 1, far_send.at[t], far_recv.at[t], behind_at)

    def near_back(t):
        return give_back(t, 2, near_send.at[t], near_recv.at[t], behind_at)

    def counts_to(r):
        return [
            remote(
                count_send.at[r], count_recv.at[r, j], csend_sem.at[j], crecv_sem.at[r, j], partner
            )
            for j, partner in enumerate(partners[r])
        ]

    def load(t, which):
        k_from, v_from = (k_prev, v_prev) if t < kv_heads else (k_next, v_next)
        src = (k_from, v_from)[which]
        columns = slice((t % kv_heads) * HEAD_DIM, (t % kv_heads + 1) * HEAD_DIM)
        return pltpu.make_async_copy(
            src.at[:, columns], held.at[t, 0, which], load_sem.at[int(t >= AHEAD)]
        )

    def wait_loads(first, last):
        part = held.at[first:last, 0]
        pltpu.make_async_copy(part, part, load_sem.at[int(first >= AHEAD)]).wait()

    def columns_of(g, count=GROUP):
        return pl.ds(pl.multiple_of(g * (count * HEAD_DIM), HEAD_DIM), count * HEAD_DIM)

    barrier = pltpu.get_barrier_semaphore()
    peers = sum(partners, [])
    for peer in peers:
        pl.semaphore_signal(barrier, inc=1, device_id=peer, device_id_type=MESH)

    @pl.when(has_next)
    def _():
        pl.semaphore_signal(barrier, inc=1, device_id={"seq": ahead_at}, device_id_type=MESH)

    @pl.when(has_behind)
    def _():
        pl.semaphore_signal(barrier, inc=1, device_id={"seq": behind_at}, device_id_type=MESH)

    for t in range(AHEAD):
        load(t, 0).start()
        load(t, 1).start()
    small = ((flags, flags_v), (seg_prev, seg_prev_v), (seg_next, seg_next_v))
    small_copies = [
        pltpu.make_async_copy(src, dst, small_sem.at[i]) for i, (src, dst) in enumerate(small)
    ]
    for copy in small_copies:
        copy.start()
    for t in range(AHEAD, chunks):
        load(t, 0).start()
        load(t, 1).start()
    for i, src in enumerate((q_prev, upstream, q_next)):
        pltpu.make_async_copy(src, arrays_v.at[i], load_sem.at[2]).start()

    def clear(ref, *at):
        def one(t, carry):
            ref[(t, *at)] = jnp.zeros(ref.shape[1 + len(at) :], ref.dtype)
            return carry

        lax.fori_loop(0, ref.shape[0], one, 0)

    @pl.when(chip_at == 0)
    def _():
        clear(held, 1)
        clear(far_recv)

    @pl.when(chip_at <= 1)
    def _():
        clear(held, 2)

    @pl.when(chip_at == last_chip)
    def _():
        clear(far_recv)
        clear(near_recv)

    wait_loads(0, AHEAD)
    ends = chip_at // last_chip + (last_chip - chip_at) // last_chip
    pl.semaphore_wait(barrier, len(peers) + 2 - ends)

    @pl.when(has_next)
    def _():
        for t in range(AHEAD):
            own_ahead(t).start()

    for copy in small_copies:
        copy.wait()
    count_send[0] = jnp.broadcast_to(
        jnp.sum(flags_v[...].astype(F32), axis=1, keepdims=True), count_send.shape[1:]
    )

    rows_at = lax.broadcasted_iota(jnp.int32, (HEAD_DIM, HEAD_DIM), 0)
    lanes_at = lax.broadcasted_iota(jnp.int32, (HEAD_DIM, HEAD_DIM), 1)
    for m, seg in enumerate((seg_prev_v, seg_next_v)):
        def ids_at(index, seg=seg):
            return seg[:, pl.ds(pl.multiple_of(index * HEAD_DIM, HEAD_DIM), HEAD_DIM)].astype(F32)

        q_ids = ids_at(seq_at)
        for d in range(BLOCKS):
            k_ids = column_of(ids_at((seq_at + n_seq - d) % n_seq))
            keep = k_ids == q_ids
            if d == 0:
                keep = keep & (rows_at <= lanes_at)
                block_bias = jnp.where(keep, 0.0, -1e30)
            else:
                block_bias = jnp.where(keep, 0.0, -1e30)
                block_bias = jnp.where(seq_at >= d, block_bias, -1e30)
            bias[m, d * HEAD_DIM : (d + 1) * HEAD_DIM, :] = block_bias

    for copy in counts_to(0):
        copy.start()
    wait_loads(AHEAD, chunks)
    pltpu.make_async_copy(arrays_v, arrays_v, load_sem.at[2]).wait()

    def window(w, which):
        return jnp.concatenate(
            [held[w, 0, which], side[w, 1 - core, which], held[w, 1, which],
             side[w, 2 - core, which], held[w, 2, which]],
            axis=0,
        )

    def stacked(i, g, first, count):
        return jnp.concatenate(
            [
                arrays_v[i, :, pl.ds(pl.multiple_of(g * width + j * HEAD_DIM, HEAD_DIM), HEAD_DIM)]
                for j in range(first, first + count)
            ],
            axis=0,
        )

    def expo(k_all, q_part, m):
        pair = bias[m]
        scores = dot(k_all, q_part, ((1,), (1,))) + jnp.concatenate([pair, pair], axis=1)
        top = over_keys(scores, jnp.maximum, jnp.max)
        values = jnp.exp2((scores - top) * (scale * math.log2(math.e)))
        return values, 1.0 / over_keys(values, jnp.add, jnp.sum)

    def backward(w):
        k_all, v_all = window(w, 0), window(w, 1)
        k_turned = jnp.transpose(k_all)
        flag_row = flags_v[...].astype(F32)
        flag_pair = jnp.concatenate([flag_row, flag_row], axis=1)
        dk = dv = None
        for half in range(2):
            q_part = stacked(0, w, 2 * half, 2)
            u_part = stacked(1, w, 2 * half, 2)
            values, inverse = expo(k_all, q_part, 0)
            d_probs = dot(v_all, u_part, ((1,), (1,)))
            row_delta = over_keys(values * d_probs, jnp.add, jnp.sum) * inverse
            probs = values * (inverse * flag_pair)
            d_scores = (probs * (d_probs - row_delta)).astype(BF16)
            dq_t[w, :, half * 256 : (half + 1) * 256] = dot(k_turned, d_scores, ((1,), (0,)))
            dk_part = dot(d_scores, q_part, ((1,), (0,)))
            dv_part = dot(probs.astype(BF16), u_part, ((1,), (0,)))
            dk = dk_part if dk is None else dk + dk_part
            dv = dv_part if dv is None else dv + dv_part
        for which, total in enumerate((dk, dv)):
            for d in range(BLOCKS):
                block = total[d * HEAD_DIM : (d + 1) * HEAD_DIM]
                if d % 2:
                    side_grads[w, d // 2, which] = block.astype(BF16)
                else:
                    grads[w, d // 2, which] = block

    def forward(w):
        g = w - kv_heads
        k_all, v_all = window(w, 0), window(w, 1)
        lower = jnp.concatenate([rows_at <= lanes_at] * GROUP, axis=1)
        scores = dot(k_all, stacked(2, g, 0, GROUP), ((1,), (1,)))
        scores = scores + jnp.concatenate([bias[1]] * GROUP, axis=1)
        blocks = [scores[d * HEAD_DIM : (d + 1) * HEAD_DIM] for d in range(BLOCKS)]
        blocks = [jnp.where(lower, blocks[0], blocks[4])] + blocks[1:4]
        top = jnp.max(functools.reduce(jnp.maximum, blocks), axis=0, keepdims=True)
        values = [jnp.exp2((x - top) * (scale * math.log2(math.e))) for x in blocks]
        inverse = 1.0 / jnp.sum(functools.reduce(jnp.add, values), axis=0, keepdims=True)
        ends = jnp.where(lower, values[0], 0.0), jnp.where(lower, 0.0, values[0])
        parts = [x.astype(BF16) for x in [ends[0]] + values[1:] + [ends[1]]]
        mixed = dot(jnp.transpose(v_all), jnp.concatenate(parts, axis=0), ((1,), (0,))) * inverse
        for j in range(GROUP):
            at = pl.multiple_of(g * width + j * HEAD_DIM, HEAD_DIM)
            attn_v[:, pl.ds(at, HEAD_DIM)] = jnp.transpose(
                mixed[:, j * HEAD_DIM : (j + 1) * HEAD_DIM]
            ).astype(BF16)

    def factor_row():
        total = count_send[rounds, 0:1, :]
        return (HEAD_DIM * n_fsdp * n_seq) / jnp.maximum(total, 1.0)

    def finish_q(g):
        gain = factor_row() * scale
        for j in range(GROUP):
            at = pl.multiple_of(g * width + j * HEAD_DIM, HEAD_DIM)
            turned = jnp.transpose(dq_t[g, :, j * HEAD_DIM : (j + 1) * HEAD_DIM])
            gq_v[:, pl.ds(at, HEAD_DIM)] = (turned * gain).astype(BF16)

    def take_side(w):
        for part in range(2):
            grads[w, core + part] = grads[w, core + part] + side_recv[w, part].astype(F32)
        far_send[w] = grads[w, 2].astype(BF16)

    def take_far(w):
        near_send[w] = (grads[w, 1] + far_recv[w].astype(F32)).astype(BF16)

    def take_near(w):
        total = grads[w, 0] + near_recv[w].astype(F32)
        gain = factor_row()
        gk_v[:, columns_of(w, 1)] = (total[0] * (gain * scale)).astype(BF16)
        gv_v[:, columns_of(w, 1)] = (total[1] * gain).astype(BF16)

    def during(t, first, count, also=None):
        here = (t >= first) & (t < first + count)
        return pl.when(here if also is None else here & also)

    both_sides = has_next & has_behind

    late = max(LAG + kv_heads // 2 + 8, COUNT_STEPS * rounds + 3)

    def one_step(t, carry):
        @during(t, 0, chunks - AHEAD, has_next)
        def _():
            own_ahead(t + AHEAD).start()

        @during(t, 0, chunks, has_behind)
        def _():
            own_ahead(t).wait_recv()

        @during(t, 0, chunks, both_sides)
        def _():
            near_ahead(t).start()

        @during(t, LAG - 1, chunks, chip_at > 1)
        def _():
            near_ahead(t - LAG + 1).wait_recv()

        @during(t, LAG - 1, chunks)
        def _():
            all_side(t - LAG + 1).start()

        @during(t, LAG + 1, kv_heads)
        def _():
            grads_side(t - LAG - 1).start()

        @during(t, LAG + 2, kv_heads)
        def _():
            grads_side(t - LAG - 2).wait_recv()
            take_side(t - LAG - 2)

        @during(t, LAG + 5, kv_heads, both_sides)
        def _():
            far_back(t - LAG - 5).wait_recv()

        @during(t, LAG + 5, kv_heads)
        def _():
            take_far(t - LAG - 5)

        for r in range(rounds):
            @pl.when(t == COUNT_STEPS * (r + 1) - 1)
            def _(r=r):
                total = count_send[r]
                for j, copy in enumerate(counts_to(r)):
                    copy.wait()
                    total = total + count_recv[r, j]
                count_send[r + 1] = total

        @during(t, LAG, chunks)
        def _():
            all_side(t - LAG).wait_recv()

        @during(t, LAG, kv_heads)
        def _():
            backward(t - LAG)

        @during(t, LAG + kv_heads, kv_heads)
        def _():
            forward(t - LAG)

        @during(t, late - 4, kv_heads // 2)
        def _():
            for which in range(2):
                finish_q(2 * (t - late + 4) + which)

        @during(t, LAG + 2, kv_heads, chip_at > 1)
        def _():
            far_back(t - LAG - 2).start()

        @during(t, LAG + 5, kv_heads, has_behind)
        def _():
            near_back(t - LAG - 5).start()

        for r in range(1, rounds):
            @pl.when(t == COUNT_STEPS * r - 1)
            def _(r=r):
                for copy in counts_to(r):
                    copy.start()

        @during(t, late, kv_heads // 2, has_next)
        def _():
            for which in range(2):
                near_back(2 * (t - late) + which).wait_recv()

        @during(t, late, kv_heads // 2)
        def _():
            for which in range(2):
                take_near(2 * (t - late) + which)

        @during(t, LAG, chunks, has_next)
        def _():
            own_ahead(t - LAG).wait_send()

        @during(t, LAG, chunks, both_sides)
        def _():
            near_ahead(t - LAG).wait_send()

        @during(t, LAG, chunks)
        def _():
            all_side(t - LAG).wait_send()

        @during(t, LAG + 8, kv_heads)
        def _():
            grads_side(t - LAG - 8).wait_send()

        @during(t, LAG + 8, kv_heads, chip_at > 1)
        def _():
            far_back(t - LAG - 8).wait_send()

        @during(t, LAG + 8, kv_heads, has_behind)
        def _():
            near_back(t - LAG - 8).wait_send()

        return carry

    steps = max(chunks + LAG, late + kv_heads // 2, kv_heads + LAG + 8, COUNT_STEPS * rounds + 1)
    lax.fori_loop(0, steps, one_step, 0)


def write_out(*refs):
    ins, outs, sems = refs[:4], refs[4:8], refs[8]
    copies = [pltpu.make_async_copy(ins[i], outs[i], sems.at[i]) for i in range(4)]
    for copy in copies:
        copy.start()
    for copy in copies:
        copy.wait()


def count_plan(n_fsdp, n_seq):
    plan = []
    for axis, size in (("seq", n_seq), ("fsdp", n_fsdp)):
        stride = 1
        while stride < size:
            radix = min(8, size // stride)
            plan.append((axis, stride, radix))
            stride *= radix
    first = plan.pop(0)
    return [first] + plan[::-1]


def body(n_fsdp, n_seq, *args):
    q, k = args[0], args[1]
    rows = q.shape[0]
    kv_heads = k.shape[1] // HEAD_DIM
    chunks = 2 * kv_heads
    width = q.shape[1]
    plan = count_plan(n_fsdp, n_seq)
    rounds, most = len(plan), max(radix for _, _, radix in plan) - 1
    tile = (2, HEAD_DIM, HEAD_DIM)
    anywhere = pl.BlockSpec(memory_space=pl.ANY)
    vmem = pl.BlockSpec(memory_space=pltpu.VMEM)
    dma = pltpu.SemaphoreType.DMA
    done = pl.pallas_call(
        functools.partial(kernel, (kv_heads, n_fsdp, n_seq, plan)),
        out_shape=tuple(pltpu.VMEM(x.shape, BF16) for x in (q, q, k, k)),
        in_specs=[pl.BlockSpec(memory_space=pltpu.HBM)] * 10,
        out_specs=(vmem,) * 4,
        scratch_shapes=[
            pltpu.VMEM((chunks, 3) + tile, BF16),
            pltpu.VMEM((chunks, 3) + tile, BF16),
            pltpu.VMEM((kv_heads, 2) + tile, BF16),
            pltpu.VMEM((kv_heads, 2) + tile, BF16),
            pltpu.VMEM((kv_heads, 3) + tile, F32),
            pltpu.VMEM((kv_heads,) + tile, BF16),
            pltpu.VMEM((kv_heads,) + tile, BF16),
            pltpu.VMEM((kv_heads,) + tile, BF16),
            pltpu.VMEM((kv_heads,) + tile, BF16),
            pltpu.VMEM((3, rows, width), BF16),
            pltpu.VMEM(args[9].shape, jnp.int32),
            pltpu.VMEM(args[7].shape, jnp.int32),
            pltpu.VMEM(args[3].shape, jnp.int32),
            pltpu.VMEM((kv_heads, HEAD_DIM, GROUP * HEAD_DIM), F32),
            pltpu.VMEM((2, BLOCKS * HEAD_DIM, HEAD_DIM), F32),
            pltpu.VMEM((rounds + 1, 8, 128), F32),
            pltpu.VMEM((rounds, most, 8, 128), F32),
            dma((3,)),
            dma((3,)),
            dma((3, TURNS)),
            dma((3, chunks)),
            dma((3, TURNS)),
            dma((3, kv_heads)),
            dma((most,)),
            dma((rounds, most)),
        ],
        compiler_params=pltpu.CompilerParams(
            collective_id=0, has_side_effects=True, vmem_limit_bytes=60 * 1024 * 1024
        ),
    )(*args)
    return pl.pallas_call(
        write_out,
        out_shape=tuple(jax.ShapeDtypeStruct(x.shape, BF16) for x in (q, q, k, k)),
        in_specs=[anywhere] * 4,
        out_specs=(anywhere,) * 4,
        scratch_shapes=[dma((4,))],
        compiler_params=pltpu.CompilerParams(vmem_limit_bytes=8 * 1024 * 1024),
    )(*(pltpu.with_memory_space_constraint(x, pltpu.VMEM) for x in done))


def solution(mesh):
    both = P(("fsdp", "seq"), None)
    ids = P("fsdp", None)
    return jax.shard_map(
        functools.partial(body, mesh.shape["fsdp"], mesh.shape["seq"]),
        mesh=mesh,
        in_specs=(both, both, both, ids, both, both, both, ids, both, P("fsdp", "seq")),
        out_specs=(both,) * 4,
        check_vma=False,
    )
```

```python
import functools
import math

import jax
import jax.numpy as jnp
from jax import lax
from jax.experimental import pallas as pl
from jax.experimental.pallas import tpu as pltpu
from jax.sharding import PartitionSpec as P

HEAD_DIM = 128
GROUP = 4
BLOCKS = 5
AHEAD = 2
ROW_AT, TOTAL_AT = 8, 11
TURNS = 8
LAG = 4
MESH = pl.DeviceIdType.MESH
F32 = jnp.float32
BF16 = jnp.bfloat16


def dot(a, b, dims):
    return lax.dot_general(a, b, (dims, ((), ())), preferred_element_type=F32)


def over_keys(values, join, reduce):
    blocks = [values[d * HEAD_DIM : (d + 1) * HEAD_DIM] for d in range(BLOCKS)]
    return reduce(functools.reduce(join, blocks), axis=0, keepdims=True)


def column_of(row):
    return jnp.transpose(jnp.broadcast_to(row, (128, row.shape[1])))


def kernel(
    sizes,
    q_next, k_next, v_next, seg_next, q_prev, k_prev, v_prev, seg_prev, upstream, flags,
    attn_v, gq_v, gk_v, gv_v,
    held, side, side_grads, side_recv, grads, far_send, far_recv, near_send, near_recv,
    arrays_v, flags_v, seg_prev_v, seg_next_v, dq_t, bias,
    count, row_counts, row_count, hub_counts, total_made, total_count,
    load_sem, small_sem, send_sem, recv_sem, gsend_sem, grecv_sem,
    count_sem, row_sem, across_sem, hub_sem, out_sem,
):
    kv_heads, n_fsdp, n_seq = sizes
    chunks = 2 * kv_heads
    width = GROUP * HEAD_DIM
    seq_at = lax.axis_index("seq")
    fsdp_at = lax.axis_index("fsdp")
    core = seq_at % 2
    ahead_at = (seq_at + 2) % n_seq
    behind_at = (seq_at + n_seq - 2) % n_seq
    side_at = seq_at + 1 - 2 * core
    chip_at, last_chip = seq_at // 2, n_seq // 2 - 1
    has_next, has_behind = chip_at < last_chip, chip_at > 0
    scale = HEAD_DIM ** -0.5

    is_hub = seq_at == 0
    hub_one = (n_seq - seq_at) // n_seq
    middle = n_seq // 4

    def remote(src, dst, sent, received, device):
        return pltpu.make_async_remote_copy(
            src_ref=src, dst_ref=dst, send_sem=sent, recv_sem=received,
            device_id=device, device_id_type=MESH,
        )

    def pass_on(t, kind, src, dst, device):
        return remote(
            src, dst, send_sem.at[kind, t % TURNS], recv_sem.at[kind, t], {"seq": device}
        )

    def own_ahead(t):
        return pass_on(t, 0, held.at[t, 0], held.at[t, 1], ahead_at)

    def near_ahead(t):
        return pass_on(t, 1, held.at[t, 1], held.at[t, 2], ahead_at)

    def all_side(t):
        return pass_on(t, 2, held.at[t], side.at[t], side_at)

    def give_back(t, kind, src, dst, device):
        return remote(
            src, dst, gsend_sem.at[kind, t % TURNS], grecv_sem.at[kind, t], {"seq": device}
        )

    def grads_side(t):
        return give_back(t, 0, side_grads.at[t], side_recv.at[t], side_at)

    def far_back(t):
        return give_back(t, 1, far_send.at[t], far_recv.at[t], behind_at)

    def near_back(t):
        return give_back(t, 2, near_send.at[t], near_recv.at[t], behind_at)

    def count_in():
        return remote(count, row_counts.at[seq_at], count_sem.at[0], row_sem.at[seq_at], {"seq": 0})

    def row_arrival(i):
        return remote(count, row_counts.at[i], count_sem.at[0], row_sem.at[i], {"seq": 0})

    def count_across(j):
        return remote(
            row_count, hub_counts.at[j], across_sem.at[j], hub_sem.at[j],
            {"fsdp": (fsdp_at + j) % n_fsdp},
        )

    def count_out(i):
        return remote(total_made, total_count, out_sem.at[i], count_sem.at[1], {"seq": i})

    def count_behind():
        return remote(
            total_count, total_count, out_sem.at[0], count_sem.at[1], {"seq": behind_at}
        )

    def load(t, which):
        k_from, v_from = (k_prev, v_prev) if t < kv_heads else (k_next, v_next)
        src = (k_from, v_from)[which]
        columns = slice((t % kv_heads) * HEAD_DIM, (t % kv_heads + 1) * HEAD_DIM)
        return pltpu.make_async_copy(
            src.at[:, columns], held.at[t, 0, which], load_sem.at[int(t >= AHEAD)]
        )

    def wait_loads(first, last):
        part = held.at[first:last, 0]
        pltpu.make_async_copy(part, part, load_sem.at[int(first >= AHEAD)]).wait()

    def columns_of(g, count=GROUP):
        return pl.ds(pl.multiple_of(g * (count * HEAD_DIM), HEAD_DIM), count * HEAD_DIM)

    barrier = pltpu.get_barrier_semaphore()
    pl.semaphore_signal(barrier, inc=1, device_id={"seq": side_at}, device_id_type=MESH)

    @pl.when(has_next)
    def _():
        pl.semaphore_signal(barrier, inc=1, device_id={"seq": ahead_at}, device_id_type=MESH)

    @pl.when(has_behind)
    def _():
        pl.semaphore_signal(barrier, inc=1, device_id={"seq": behind_at}, device_id_type=MESH)

    @pl.when(is_hub)
    def _():
        def one(i, carry):
            pl.semaphore_signal(barrier, inc=1, device_id={"seq": i}, device_id_type=MESH)
            return carry

        lax.fori_loop(1, n_seq, one, 0)
        for j in range(1, n_fsdp):
            pl.semaphore_signal(
                barrier, inc=1, device_id={"fsdp": (fsdp_at + j) % n_fsdp}, device_id_type=MESH
            )

    for t in range(AHEAD):
        load(t, 0).start()
        load(t, 1).start()
    small = ((flags, flags_v), (seg_prev, seg_prev_v), (seg_next, seg_next_v))
    small_copies = [
        pltpu.make_async_copy(src, dst, small_sem.at[i]) for i, (src, dst) in enumerate(small)
    ]
    for copy in small_copies:
        copy.start()
    for t in range(AHEAD, chunks):
        load(t, 0).start()
        load(t, 1).start()
    for i, src in enumerate((q_prev, upstream, q_next)):
        pltpu.make_async_copy(src, arrays_v.at[i], load_sem.at[2]).start()

    def clear(ref, *at):
        def one(t, carry):
            ref[(t, *at)] = jnp.zeros(ref.shape[1 + len(at) :], ref.dtype)
            return carry

        lax.fori_loop(0, ref.shape[0], one, 0)

    @pl.when(chip_at == 0)
    def _():
        clear(held, 1)
        clear(far_recv)

    @pl.when(chip_at <= 1)
    def _():
        clear(held, 2)

    @pl.when(chip_at == last_chip)
    def _():
        clear(far_recv)
        clear(near_recv)

    wait_loads(0, AHEAD)
    ends = chip_at // last_chip + (last_chip - chip_at) // last_chip
    pl.semaphore_wait(barrier, 4 - ends + hub_one * (n_fsdp - 2))

    @pl.when(has_next)
    def _():
        for t in range(AHEAD):
            own_ahead(t).start()

    for copy in small_copies:
        copy.wait()
    count[...] = jnp.broadcast_to(
        jnp.sum(flags_v[...].astype(F32), axis=1, keepdims=True), count.shape
    )

    rows_at = lax.broadcasted_iota(jnp.int32, (HEAD_DIM, HEAD_DIM), 0)
    lanes_at = lax.broadcasted_iota(jnp.int32, (HEAD_DIM, HEAD_DIM), 1)
    for m, seg in enumerate((seg_prev_v, seg_next_v)):
        def ids_at(index, seg=seg):
            return seg[:, pl.ds(pl.multiple_of(index * HEAD_DIM, HEAD_DIM), HEAD_DIM)].astype(F32)

        q_ids = ids_at(seq_at)
        for d in range(BLOCKS):
            k_ids = column_of(ids_at((seq_at + n_seq - d) % n_seq))
            keep = k_ids == q_ids
            if d == 0:
                keep = keep & (rows_at <= lanes_at)
                block_bias = jnp.where(keep, 0.0, -1e30)
            else:
                block_bias = jnp.where(keep, 0.0, -1e30)
                block_bias = jnp.where(seq_at >= d, block_bias, -1e30)
            bias[m, d * HEAD_DIM : (d + 1) * HEAD_DIM, :] = block_bias

    @pl.when(seq_at > 0)
    def _():
        count_in().start()

    wait_loads(AHEAD, chunks)
    pltpu.make_async_copy(arrays_v, arrays_v, load_sem.at[2]).wait()

    def window(w, which):
        return jnp.concatenate(
            [held[w, 0, which], side[w, 1 - core, which], held[w, 1, which],
             side[w, 2 - core, which], held[w, 2, which]],
            axis=0,
        )

    def stacked(i, g, first, count):
        return jnp.concatenate(
            [
                arrays_v[i, :, pl.ds(pl.multiple_of(g * width + j * HEAD_DIM, HEAD_DIM), HEAD_DIM)]
                for j in range(first, first + count)
            ],
            axis=0,
        )

    def expo(k_all, q_part, m):
        pair = bias[m]
        scores = dot(k_all, q_part, ((1,), (1,))) + jnp.concatenate([pair, pair], axis=1)
        top = over_keys(scores, jnp.maximum, jnp.max)
        values = jnp.exp2((scores - top) * (scale * math.log2(math.e)))
        return values, 1.0 / over_keys(values, jnp.add, jnp.sum)

    def backward(w):
        k_all, v_all = window(w, 0), window(w, 1)
        k_turned = jnp.transpose(k_all)
        flag_row = flags_v[...].astype(F32)
        flag_pair = jnp.concatenate([flag_row, flag_row], axis=1)
        dk = dv = None
        for half in range(2):
            q_part = stacked(0, w, 2 * half, 2)
            u_part = stacked(1, w, 2 * half, 2)
            values, inverse = expo(k_all, q_part, 0)
            d_probs = dot(v_all, u_part, ((1,), (1,)))
            row_delta = over_keys(values * d_probs, jnp.add, jnp.sum) * inverse
            probs = values * (inverse * flag_pair)
            d_scores = (probs * (d_probs - row_delta)).astype(BF16)
            dq_t[w, :, half * 256 : (half + 1) * 256] = dot(k_turned, d_scores, ((1,), (0,)))
            dk_part = dot(d_scores, q_part, ((1,), (0,)))
            dv_part = dot(probs.astype(BF16), u_part, ((1,), (0,)))
            dk = dk_part if dk is None else dk + dk_part
            dv = dv_part if dv is None else dv + dv_part
        for which, total in enumerate((dk, dv)):
            for d in range(BLOCKS):
                block = total[d * HEAD_DIM : (d + 1) * HEAD_DIM]
                if d % 2:
                    side_grads[w, d // 2, which] = block.astype(BF16)
                else:
                    grads[w, d // 2, which] = block

    def forward(w):
        g = w - kv_heads
        k_all, v_all = window(w, 0), window(w, 1)
        lower = jnp.concatenate([rows_at <= lanes_at] * GROUP, axis=1)
        scores = dot(k_all, stacked(2, g, 0, GROUP), ((1,), (1,)))
        scores = scores + jnp.concatenate([bias[1]] * GROUP, axis=1)
        blocks = [scores[d * HEAD_DIM : (d + 1) * HEAD_DIM] for d in range(BLOCKS)]
        blocks = [jnp.where(lower, blocks[0], blocks[4])] + blocks[1:4]
        top = jnp.max(functools.reduce(jnp.maximum, blocks), axis=0, keepdims=True)
        values = [jnp.exp2((x - top) * (scale * math.log2(math.e))) for x in blocks]
        inverse = 1.0 / jnp.sum(functools.reduce(jnp.add, values), axis=0, keepdims=True)
        ends = jnp.where(lower, values[0], 0.0), jnp.where(lower, 0.0, values[0])
        parts = [x.astype(BF16) for x in [ends[0]] + values[1:] + [ends[1]]]
        mixed = dot(jnp.transpose(v_all), jnp.concatenate(parts, axis=0), ((1,), (0,))) * inverse
        for j in range(GROUP):
            at = pl.multiple_of(g * width + j * HEAD_DIM, HEAD_DIM)
            attn_v[:, pl.ds(at, HEAD_DIM)] = jnp.transpose(
                mixed[:, j * HEAD_DIM : (j + 1) * HEAD_DIM]
            ).astype(BF16)

    def factor_row():
        total = total_count[0:1, :]
        return (HEAD_DIM * n_fsdp * n_seq) / jnp.maximum(total, 1.0)

    def finish_q(g):
        gain = factor_row() * scale
        for j in range(GROUP):
            at = pl.multiple_of(g * width + j * HEAD_DIM, HEAD_DIM)
            turned = jnp.transpose(dq_t[g, :, j * HEAD_DIM : (j + 1) * HEAD_DIM])
            gq_v[:, pl.ds(at, HEAD_DIM)] = (turned * gain).astype(BF16)

    def take_side(w):
        for part in range(2):
            grads[w, core + part] = grads[w, core + part] + side_recv[w, part].astype(F32)
        far_send[w] = grads[w, 2].astype(BF16)

    def take_far(w):
        near_send[w] = (grads[w, 1] + far_recv[w].astype(F32)).astype(BF16)

    def take_near(w):
        total = grads[w, 0] + near_recv[w].astype(F32)
        gain = factor_row()
        gk_v[:, columns_of(w, 1)] = (total[0] * (gain * scale)).astype(BF16)
        gv_v[:, columns_of(w, 1)] = (total[1] * gain).astype(BF16)

    def during(t, first, count, also=None):
        here = (t >= first) & (t < first + count)
        return pl.when(here if also is None else here & also)

    both_sides = has_next & has_behind

    late = max(LAG + kv_heads // 2 + 8, TOTAL_AT + 5)

    def one_step(t, carry):
        @during(t, 0, chunks - AHEAD, has_next)
        def _():
            own_ahead(t + AHEAD).start()

        @during(t, 0, chunks, has_behind)
        def _():
            own_ahead(t).wait_recv()

        @during(t, 0, chunks, both_sides)
        def _():
            near_ahead(t).start()

        @during(t, LAG - 1, chunks, chip_at > 1)
        def _():
            near_ahead(t - LAG + 1).wait_recv()

        @during(t, LAG - 1, chunks)
        def _():
            all_side(t - LAG + 1).start()

        @during(t, LAG + 1, kv_heads)
        def _():
            grads_side(t - LAG - 1).start()

        @during(t, LAG + 2, kv_heads)
        def _():
            grads_side(t - LAG - 2).wait_recv()
            take_side(t - LAG - 2)

        @during(t, LAG + 5, kv_heads, both_sides)
        def _():
            far_back(t - LAG - 5).wait_recv()

        @during(t, LAG + 5, kv_heads)
        def _():
            take_far(t - LAG - 5)

        @pl.when((t == ROW_AT) & is_hub)
        def _():
            def one(i, total):
                row_arrival(i).wait_recv()
                return total + row_counts[i]

            row_count[...] = lax.fori_loop(1, n_seq, one, count[...])

        @pl.when((t == TOTAL_AT) & is_hub)
        def _():
            total = row_count[...]
            for j in range(1, n_fsdp):
                count_across(j).wait()
                total = total + hub_counts[j]
            total_made[...] = total
            total_count[...] = total

        @pl.when((t == TOTAL_AT) & (seq_at > 0) & (chip_at != middle))
        def _():
            count_out(0).wait_recv()
            count_in().wait_send()

        @pl.when((t == TOTAL_AT + 1) & (chip_at == middle))
        def _():
            count_behind().wait_recv()
            count_in().wait_send()

        @during(t, LAG, chunks)
        def _():
            all_side(t - LAG).wait_recv()

        @during(t, LAG, kv_heads)
        def _():
            backward(t - LAG)

        @during(t, LAG + kv_heads, kv_heads)
        def _():
            forward(t - LAG)

        @during(t, late - 4, kv_heads // 2)
        def _():
            for which in range(2):
                finish_q(2 * (t - late + 4) + which)

        @during(t, LAG + 2, kv_heads, chip_at > 1)
        def _():
            far_back(t - LAG - 2).start()

        @during(t, LAG + 5, kv_heads, has_behind)
        def _():
            near_back(t - LAG - 5).start()

        @pl.when((t == ROW_AT) & is_hub)
        def _():
            for j in range(1, n_fsdp):
                count_across(j).start()

        @pl.when((t == TOTAL_AT) & is_hub)
        def _():
            def one(i, carry):
                count_out(i).start()
                return carry

            lax.fori_loop(1, 2 * middle, one, 0)
            lax.fori_loop(2 * middle + 2, n_seq, one, 0)

        @pl.when((t == TOTAL_AT) & (chip_at == middle + 1))
        def _():
            count_behind().start()

        @pl.when((t == TOTAL_AT + 2) & (chip_at == middle + 1))
        def _():
            count_behind().wait_send()

        @pl.when((t == TOTAL_AT + 2) & is_hub)
        def _():
            def one(i, carry):
                count_out(i).wait_send()
                return carry

            lax.fori_loop(1, 2 * middle, one, 0)
            lax.fori_loop(2 * middle + 2, n_seq, one, 0)

        @during(t, late, kv_heads // 2, has_next)
        def _():
            for which in range(2):
                near_back(2 * (t - late) + which).wait_recv()

        @during(t, late, kv_heads // 2)
        def _():
            for which in range(2):
                take_near(2 * (t - late) + which)

        @during(t, LAG, chunks, has_next)
        def _():
            own_ahead(t - LAG).wait_send()

        @during(t, LAG, chunks, both_sides)
        def _():
            near_ahead(t - LAG).wait_send()

        @during(t, LAG, chunks)
        def _():
            all_side(t - LAG).wait_send()

        @during(t, LAG + 8, kv_heads)
        def _():
            grads_side(t - LAG - 8).wait_send()

        @during(t, LAG + 8, kv_heads, chip_at > 1)
        def _():
            far_back(t - LAG - 8).wait_send()

        @during(t, LAG + 8, kv_heads, has_behind)
        def _():
            near_back(t - LAG - 8).wait_send()

        return carry

    steps = max(chunks + LAG, late + kv_heads // 2, kv_heads + LAG + 8, TOTAL_AT + 3)
    lax.fori_loop(0, steps, one_step, 0)


def write_out(*refs):
    ins, outs, sems = refs[:4], refs[4:8], refs[8]
    copies = [pltpu.make_async_copy(ins[i], outs[i], sems.at[i]) for i in range(4)]
    for copy in copies:
        copy.start()
    for copy in copies:
        copy.wait()


def body(n_fsdp, n_seq, *args):
    q, k = args[0], args[1]
    rows = q.shape[0]
    kv_heads = k.shape[1] // HEAD_DIM
    chunks = 2 * kv_heads
    width = q.shape[1]
    tile = (2, HEAD_DIM, HEAD_DIM)
    anywhere = pl.BlockSpec(memory_space=pl.ANY)
    vmem = pl.BlockSpec(memory_space=pltpu.VMEM)
    dma = pltpu.SemaphoreType.DMA
    done = pl.pallas_call(
        functools.partial(kernel, (kv_heads, n_fsdp, n_seq)),
        out_shape=tuple(pltpu.VMEM(x.shape, BF16) for x in (q, q, k, k)),
        in_specs=[pl.BlockSpec(memory_space=pltpu.HBM)] * 10,
        out_specs=(vmem,) * 4,
        scratch_shapes=[
            pltpu.VMEM((chunks, 3) + tile, BF16),
            pltpu.VMEM((chunks, 3) + tile, BF16),
            pltpu.VMEM((kv_heads, 2) + tile, BF16),
            pltpu.VMEM((kv_heads, 2) + tile, BF16),
            pltpu.VMEM((kv_heads, 3) + tile, F32),
            pltpu.VMEM((kv_heads,) + tile, BF16),
            pltpu.VMEM((kv_heads,) + tile, BF16),
            pltpu.VMEM((kv_heads,) + tile, BF16),
            pltpu.VMEM((kv_heads,) + tile, BF16),
            pltpu.VMEM((3, rows, width), BF16),
            pltpu.VMEM(args[9].shape, jnp.int32),
            pltpu.VMEM(args[7].shape, jnp.int32),
            pltpu.VMEM(args[3].shape, jnp.int32),
            pltpu.VMEM((kv_heads, HEAD_DIM, GROUP * HEAD_DIM), F32),
            pltpu.VMEM((2, BLOCKS * HEAD_DIM, HEAD_DIM), F32),
            pltpu.VMEM((8, 128), F32),
            pltpu.VMEM((n_seq, 8, 128), F32),
            pltpu.VMEM((8, 128), F32),
            pltpu.VMEM((n_fsdp, 8, 128), F32),
            pltpu.VMEM((8, 128), F32),
            pltpu.VMEM((8, 128), F32),
            dma((3,)),
            dma((3,)),
            dma((3, TURNS)),
            dma((3, chunks)),
            dma((3, TURNS)),
            dma((3, kv_heads)),
            dma((2,)),
            dma((n_seq,)),
            dma((n_fsdp,)),
            dma((n_fsdp,)),
            dma((n_seq,)),
        ],
        compiler_params=pltpu.CompilerParams(
            collective_id=0, has_side_effects=True, vmem_limit_bytes=60 * 1024 * 1024
        ),
    )(*args)
    return pl.pallas_call(
        write_out,
        out_shape=tuple(jax.ShapeDtypeStruct(x.shape, BF16) for x in (q, q, k, k)),
        in_specs=[anywhere] * 4,
        out_specs=(anywhere,) * 4,
        scratch_shapes=[dma((4,))],
        compiler_params=pltpu.CompilerParams(vmem_limit_bytes=8 * 1024 * 1024),
    )(*(pltpu.with_memory_space_constraint(x, pltpu.VMEM) for x in done))


def solution(mesh):
    both = P(("fsdp", "seq"), None)
    ids = P("fsdp", None)
    return jax.shard_map(
        functools.partial(body, mesh.shape["fsdp"], mesh.shape["seq"]),
        mesh=mesh,
        in_specs=(both, both, both, ids, both, both, both, ids, both, P("fsdp", "seq")),
        out_specs=(both,) * 4,
        check_vma=False,
    )
```

```python
import functools
import math

import jax
import jax.numpy as jnp
from jax import lax
from jax.experimental import pallas as pl
from jax.experimental.pallas import tpu as pltpu
from jax.sharding import PartitionSpec as P

HEAD_DIM = 128
GROUP = 4
BLOCKS = 5
AHEAD = 2
ROW_AT, TOTAL_AT = 8, 11
TURNS = 8
BACK_TURNS = 4
LAG = 4
MESH = pl.DeviceIdType.MESH
F32 = jnp.float32
BF16 = jnp.bfloat16


def dot(a, b, dims):
    return lax.dot_general(a, b, (dims, ((), ())), preferred_element_type=F32)


def over_keys(values, join, reduce):
    blocks = [values[d * HEAD_DIM : (d + 1) * HEAD_DIM] for d in range(BLOCKS)]
    return reduce(functools.reduce(join, blocks), axis=0, keepdims=True)


def column_of(row):
    return jnp.transpose(jnp.broadcast_to(row, (128, row.shape[1])))


def kernel(
    sizes,
    q_next, k_next, v_next, seg_next, q_prev, k_prev, v_prev, seg_prev, upstream, flags,
    attn_v, gq_v, gk_v, gv_v,
    held, side, side_grads, side_recv, grads, far_send, far_recv, near_send, near_recv,
    arrays_v, flags_v, seg_prev_v, seg_next_v, dq_t, bias,
    count, row_counts, row_count, hub_counts, total_made, total_count,
    load_sem, small_sem, send_sem, recv_sem, gsend_sem, grecv_sem,
    count_sem, row_sem, across_sem, hub_sem, out_sem,
):
    kv_heads, n_fsdp, n_seq = sizes
    chunks = 2 * kv_heads
    width = GROUP * HEAD_DIM
    seq_at = lax.axis_index("seq")
    fsdp_at = lax.axis_index("fsdp")
    core = seq_at % 2
    ahead_at = (seq_at + 2) % n_seq
    behind_at = (seq_at + n_seq - 2) % n_seq
    side_at = seq_at + 1 - 2 * core
    chip_at, last_chip = seq_at // 2, n_seq // 2 - 1
    has_next, has_behind = chip_at < last_chip, chip_at > 0
    scale = HEAD_DIM ** -0.5

    is_hub = seq_at == 0
    hub_one = (n_seq - seq_at) // n_seq
    middle = n_seq // 4

    def remote(src, dst, sent, received, device):
        return pltpu.make_async_remote_copy(
            src_ref=src, dst_ref=dst, send_sem=sent, recv_sem=received,
            device_id=device, device_id_type=MESH,
        )

    def pass_on(t, kind, src, dst, device):
        return remote(
            src, dst, send_sem.at[kind, t % TURNS], recv_sem.at[kind, t], {"seq": device}
        )

    def own_ahead(t):
        return pass_on(t, 0, held.at[t, 0], held.at[t, 1], ahead_at)

    def near_ahead(t):
        return pass_on(t, 1, held.at[t, 1], held.at[t, 2], ahead_at)

    def all_side(t):
        return pass_on(t, 2, held.at[t], side.at[t], side_at)

    def give_back(t, kind, src, dst, device):
        return remote(
            src, dst, gsend_sem.at[kind, t % BACK_TURNS], grecv_sem.at[kind, t], {"seq": device}
        )

    def grads_side(t):
        return give_back(t, 0, side_grads.at[t], side_recv.at[t], side_at)

    def far_back(t):
        return give_back(t, 1, far_send.at[t], far_recv.at[t], behind_at)

    def near_back(t):
        return give_back(t, 2, near_send.at[t], near_recv.at[t], behind_at)

    def count_in():
        return remote(count, row_counts.at[seq_at], count_sem.at[0], row_sem.at[seq_at], {"seq": 0})

    def row_arrival(i):
        return remote(count, row_counts.at[i], count_sem.at[0], row_sem.at[i], {"seq": 0})

    def count_across(j):
        return remote(
            row_count, hub_counts.at[j], across_sem.at[j], hub_sem.at[j],
            {"fsdp": (fsdp_at + j) % n_fsdp},
        )

    def count_out(i):
        return remote(total_made, total_count, out_sem.at[i], count_sem.at[1], {"seq": i})

    def count_behind():
        return remote(
            total_count, total_count, out_sem.at[0], count_sem.at[1], {"seq": behind_at}
        )

    def load(t, which):
        k_from, v_from = (k_prev, v_prev) if t < kv_heads else (k_next, v_next)
        src = (k_from, v_from)[which]
        columns = slice((t % kv_heads) * HEAD_DIM, (t % kv_heads + 1) * HEAD_DIM)
        return pltpu.make_async_copy(
            src.at[:, columns], held.at[t, 0, which], load_sem.at[int(t >= AHEAD)]
        )

    def wait_loads(first, last):
        part = held.at[first:last, 0]
        pltpu.make_async_copy(part, part, load_sem.at[int(first >= AHEAD)]).wait()

    def columns_of(g, count=GROUP):
        return pl.ds(pl.multiple_of(g * (count * HEAD_DIM), HEAD_DIM), count * HEAD_DIM)

    barrier = pltpu.get_barrier_semaphore()
    pl.semaphore_signal(barrier, inc=1, device_id={"seq": side_at}, device_id_type=MESH)

    @pl.when(has_next)
    def _():
        pl.semaphore_signal(barrier, inc=1, device_id={"seq": ahead_at}, device_id_type=MESH)

    @pl.when(has_behind)
    def _():
        pl.semaphore_signal(barrier, inc=1, device_id={"seq": behind_at}, device_id_type=MESH)

    @pl.when(is_hub)
    def _():
        def one(i, carry):
            pl.semaphore_signal(barrier, inc=1, device_id={"seq": i}, device_id_type=MESH)
            return carry

        lax.fori_loop(1, n_seq, one, 0)
        for j in range(1, n_fsdp):
            pl.semaphore_signal(
                barrier, inc=1, device_id={"fsdp": (fsdp_at + j) % n_fsdp}, device_id_type=MESH
            )

    for t in range(AHEAD):
        load(t, 0).start()
        load(t, 1).start()
    small = ((flags, flags_v), (seg_prev, seg_prev_v), (seg_next, seg_next_v))
    small_copies = [
        pltpu.make_async_copy(src, dst, small_sem.at[i]) for i, (src, dst) in enumerate(small)
    ]
    for copy in small_copies:
        copy.start()
    for t in range(AHEAD, chunks):
        load(t, 0).start()
        load(t, 1).start()
    for i, src in enumerate((q_prev, upstream, q_next)):
        pltpu.make_async_copy(src, arrays_v.at[i], load_sem.at[2]).start()

    def clear(ref, *at):
        def one(t, carry):
            ref[(t, *at)] = jnp.zeros(ref.shape[1 + len(at) :], ref.dtype)
            return carry

        lax.fori_loop(0, ref.shape[0], one, 0)

    @pl.when(chip_at == 0)
    def _():
        clear(held, 1)
        clear(far_recv)

    @pl.when(chip_at <= 1)
    def _():
        clear(held, 2)

    @pl.when(chip_at == last_chip)
    def _():
        clear(far_recv)
        clear(near_recv)

    wait_loads(0, AHEAD)
    ends = chip_at // last_chip + (last_chip - chip_at) // last_chip
    pl.semaphore_wait(barrier, 4 - ends + hub_one * (n_fsdp - 2))

    @pl.when(has_next)
    def _():
        for t in range(AHEAD):
            own_ahead(t).start()

    for copy in small_copies:
        copy.wait()
    count[...] = jnp.broadcast_to(
        jnp.sum(flags_v[...].astype(F32), axis=1, keepdims=True), count.shape
    )

    rows_at = lax.broadcasted_iota(jnp.int32, (HEAD_DIM, HEAD_DIM), 0)
    lanes_at = lax.broadcasted_iota(jnp.int32, (HEAD_DIM, HEAD_DIM), 1)
    for m, seg in enumerate((seg_prev_v, seg_next_v)):
        def ids_at(index, seg=seg):
            return seg[:, pl.ds(pl.multiple_of(index * HEAD_DIM, HEAD_DIM), HEAD_DIM)].astype(F32)

        q_ids = ids_at(seq_at)
        for d in range(BLOCKS):
            k_ids = column_of(ids_at((seq_at + n_seq - d) % n_seq))
            keep = k_ids == q_ids
            if d == 0:
                keep = keep & (rows_at <= lanes_at)
                block_bias = jnp.where(keep, 0.0, -1e30)
            else:
                block_bias = jnp.where(keep, 0.0, -1e30)
                block_bias = jnp.where(seq_at >= d, block_bias, -1e30)
            bias[m, d * HEAD_DIM : (d + 1) * HEAD_DIM, :] = block_bias

    @pl.when(seq_at > 0)
    def _():
        count_in().start()

    wait_loads(AHEAD, chunks)
    pltpu.make_async_copy(arrays_v, arrays_v, load_sem.at[2]).wait()

    def window(w, which):
        return jnp.concatenate(
            [held[w, 0, which], side[w, 1 - core, which], held[w, 1, which],
             side[w, 2 - core, which], held[w, 2, which]],
            axis=0,
        )

    def stacked(i, g, first, count):
        return jnp.concatenate(
            [
                arrays_v[i, :, pl.ds(pl.multiple_of(g * width + j * HEAD_DIM, HEAD_DIM), HEAD_DIM)]
                for j in range(first, first + count)
            ],
            axis=0,
        )

    def expo(k_all, q_part, m):
        pair = bias[m]
        scores = dot(k_all, q_part, ((1,), (1,))) + jnp.concatenate([pair, pair], axis=1)
        top = over_keys(scores, jnp.maximum, jnp.max)
        values = jnp.exp2((scores - top) * (scale * math.log2(math.e)))
        return values, 1.0 / over_keys(values, jnp.add, jnp.sum)

    def backward(w):
        k_all, v_all = window(w, 0), window(w, 1)
        k_turned = jnp.transpose(k_all)
        flag_row = flags_v[...].astype(F32)
        flag_pair = jnp.concatenate([flag_row, flag_row], axis=1)
        dk = dv = None
        for half in range(2):
            q_part = stacked(0, w, 2 * half, 2)
            u_part = stacked(1, w, 2 * half, 2)
            values, inverse = expo(k_all, q_part, 0)
            d_probs = dot(v_all, u_part, ((1,), (1,)))
            row_delta = over_keys(values * d_probs, jnp.add, jnp.sum) * inverse
            probs = values * (inverse * flag_pair)
            d_scores = (probs * (d_probs - row_delta)).astype(BF16)
            dq_t[w, :, half * 256 : (half + 1) * 256] = dot(k_turned, d_scores, ((1,), (0,)))
            dk_part = dot(d_scores, q_part, ((1,), (0,)))
            dv_part = dot(probs.astype(BF16), u_part, ((1,), (0,)))
            dk = dk_part if dk is None else dk + dk_part
            dv = dv_part if dv is None else dv + dv_part
        for which, total in enumerate((dk, dv)):
            for d in range(BLOCKS):
                block = total[d * HEAD_DIM : (d + 1) * HEAD_DIM]
                if d % 2:
                    side_grads[w, d // 2, which] = block.astype(BF16)
                else:
                    grads[w, d // 2, which] = block

    def forward(w):
        g = w - kv_heads
        k_all, v_all = window(w, 0), window(w, 1)
        lower = jnp.concatenate([rows_at <= lanes_at] * GROUP, axis=1)
        scores = dot(k_all, stacked(2, g, 0, GROUP), ((1,), (1,)))
        scores = scores + jnp.concatenate([bias[1]] * GROUP, axis=1)
        blocks = [scores[d * HEAD_DIM : (d + 1) * HEAD_DIM] for d in range(BLOCKS)]
        blocks = [jnp.where(lower, blocks[0], blocks[4])] + blocks[1:4]
        top = jnp.max(functools.reduce(jnp.maximum, blocks), axis=0, keepdims=True)
        values = [jnp.exp2((x - top) * (scale * math.log2(math.e))) for x in blocks]
        inverse = 1.0 / jnp.sum(functools.reduce(jnp.add, values), axis=0, keepdims=True)
        ends = jnp.where(lower, values[0], 0.0), jnp.where(lower, 0.0, values[0])
        parts = [x.astype(BF16) for x in [ends[0]] + values[1:] + [ends[1]]]
        mixed = dot(jnp.transpose(v_all), jnp.concatenate(parts, axis=0), ((1,), (0,))) * inverse
        for j in range(GROUP):
            at = pl.multiple_of(g * width + j * HEAD_DIM, HEAD_DIM)
            attn_v[:, pl.ds(at, HEAD_DIM)] = jnp.transpose(
                mixed[:, j * HEAD_DIM : (j + 1) * HEAD_DIM]
            ).astype(BF16)

    def factor_row():
        total = total_count[0:1, :]
        return (HEAD_DIM * n_fsdp * n_seq) / jnp.maximum(total, 1.0)

    def finish_q(g):
        gain = factor_row() * scale
        for j in range(GROUP):
            at = pl.multiple_of(g * width + j * HEAD_DIM, HEAD_DIM)
            turned = jnp.transpose(dq_t[g, :, j * HEAD_DIM : (j + 1) * HEAD_DIM])
            gq_v[:, pl.ds(at, HEAD_DIM)] = (turned * gain).astype(BF16)

    def take_side(w):
        for part in range(2):
            grads[w, core + part] = grads[w, core + part] + side_recv[w, part].astype(F32)
        far_send[w] = grads[w, 2].astype(BF16)

    def take_far(w):
        near_send[w] = (grads[w, 1] + far_recv[w].astype(F32)).astype(BF16)

    def take_near(w):
        total = grads[w, 0] + near_recv[w].astype(F32)
        gain = factor_row()
        gk_v[:, columns_of(w, 1)] = (total[0] * (gain * scale)).astype(BF16)
        gv_v[:, columns_of(w, 1)] = (total[1] * gain).astype(BF16)

    def during(t, first, count, also=None):
        here = (t >= first) & (t < first + count)
        return pl.when(here if also is None else here & also)

    both_sides = has_next & has_behind

    late = max(LAG + kv_heads // 2 + 8, TOTAL_AT + 5)

    def one_step(t, carry):
        @during(t, 0, chunks - AHEAD, has_next)
        def _():
            own_ahead(t + AHEAD).start()

        @during(t, 0, chunks, has_behind)
        def _():
            own_ahead(t).wait_recv()

        @during(t, 0, chunks, both_sides)
        def _():
            near_ahead(t).start()

        @during(t, LAG - 1, chunks, chip_at > 1)
        def _():
            near_ahead(t - LAG + 1).wait_recv()

        @during(t, LAG - 1, chunks)
        def _():
            all_side(t - LAG + 1).start()

        @during(t, LAG + 1, kv_heads)
        def _():
            grads_side(t - LAG - 1).start()

        @during(t, LAG + 2, kv_heads)
        def _():
            grads_side(t - LAG - 2).wait_recv()
            take_side(t - LAG - 2)

        @during(t, LAG + 5, kv_heads, both_sides)
        def _():
            far_back(t - LAG - 5).wait_recv()

        @during(t, LAG + 5, kv_heads)
        def _():
            take_far(t - LAG - 5)

        @pl.when((t == ROW_AT) & is_hub)
        def _():
            def one(i, total):
                row_arrival(i).wait_recv()
                return total + row_counts[i]

            row_count[...] = lax.fori_loop(1, n_seq, one, count[...])

        @pl.when((t == TOTAL_AT) & is_hub)
        def _():
            total = row_count[...]
            for j in range(1, n_fsdp):
                count_across(j).wait()
                total = total + hub_counts[j]
            total_made[...] = total
            total_count[...] = total

        @pl.when((t == TOTAL_AT) & (seq_at > 0) & (chip_at != middle))
        def _():
            count_out(0).wait_recv()
            count_in().wait_send()

        @pl.when((t == TOTAL_AT + 1) & (chip_at == middle))
        def _():
            count_behind().wait_recv()
            count_in().wait_send()

        @during(t, LAG, chunks)
        def _():
            all_side(t - LAG).wait_recv()

        @during(t, LAG, kv_heads)
        def _():
            backward(t - LAG)

        @during(t, LAG + kv_heads, kv_heads)
        def _():
            forward(t - LAG)

        @during(t, late - 4, kv_heads // 2)
        def _():
            for which in range(2):
                finish_q(2 * (t - late + 4) + which)

        @during(t, LAG + 2, kv_heads, chip_at > 1)
        def _():
            far_back(t - LAG - 2).start()

        @during(t, LAG + 5, kv_heads, has_behind)
        def _():
            near_back(t - LAG - 5).start()

        @pl.when((t == ROW_AT) & is_hub)
        def _():
            for j in range(1, n_fsdp):
                count_across(j).start()

        @pl.when((t == TOTAL_AT) & is_hub)
        def _():
            def one(i, carry):
                count_out(i).start()
                return carry

            lax.fori_loop(1, 2 * middle, one, 0)
            lax.fori_loop(2 * middle + 2, n_seq, one, 0)

        @pl.when((t == TOTAL_AT) & (chip_at == middle + 1))
        def _():
            count_behind().start()

        @pl.when((t == TOTAL_AT + 2) & (chip_at == middle + 1))
        def _():
            count_behind().wait_send()

        @pl.when((t == TOTAL_AT + 2) & is_hub)
        def _():
            def one(i, carry):
                count_out(i).wait_send()
                return carry

            lax.fori_loop(1, 2 * middle, one, 0)
            lax.fori_loop(2 * middle + 2, n_seq, one, 0)

        @during(t, late, kv_heads // 2, has_next)
        def _():
            for which in range(2):
                near_back(2 * (t - late) + which).wait_recv()

        @during(t, late, kv_heads // 2)
        def _():
            for which in range(2):
                take_near(2 * (t - late) + which)

        @during(t, LAG, chunks, has_next)
        def _():
            own_ahead(t - LAG).wait_send()

        @during(t, LAG, chunks, both_sides)
        def _():
            near_ahead(t - LAG).wait_send()

        @during(t, LAG, chunks)
        def _():
            all_side(t - LAG).wait_send()

        @during(t, LAG + 4, kv_heads)
        def _():
            grads_side(t - LAG - 4).wait_send()

        @during(t, LAG + 5, kv_heads, chip_at > 1)
        def _():
            far_back(t - LAG - 5).wait_send()

        @during(t, LAG + 8, kv_heads, has_behind)
        def _():
            near_back(t - LAG - 8).wait_send()

        return carry

    steps = max(chunks + LAG, late + kv_heads // 2, kv_heads + LAG + 8, TOTAL_AT + 3)
    lax.fori_loop(0, steps, one_step, 0)


def write_out(*refs):
    ins, outs, sems = refs[:4], refs[4:8], refs[8]
    copies = [pltpu.make_async_copy(ins[i], outs[i], sems.at[i]) for i in range(4)]
    for copy in copies:
        copy.start()
    for copy in copies:
        copy.wait()


def body(n_fsdp, n_seq, *args):
    q, k = args[0], args[1]
    rows = q.shape[0]
    kv_heads = k.shape[1] // HEAD_DIM
    chunks = 2 * kv_heads
    width = q.shape[1]
    tile = (2, HEAD_DIM, HEAD_DIM)
    anywhere = pl.BlockSpec(memory_space=pl.ANY)
    vmem = pl.BlockSpec(memory_space=pltpu.VMEM)
    dma = pltpu.SemaphoreType.DMA
    done = pl.pallas_call(
        functools.partial(kernel, (kv_heads, n_fsdp, n_seq)),
        out_shape=tuple(pltpu.VMEM(x.shape, BF16) for x in (q, q, k, k)),
        in_specs=[pl.BlockSpec(memory_space=pltpu.HBM)] * 10,
        out_specs=(vmem,) * 4,
        scratch_shapes=[
            pltpu.VMEM((chunks, 3) + tile, BF16),
            pltpu.VMEM((chunks, 3) + tile, BF16),
            pltpu.VMEM((kv_heads, 2) + tile, BF16),
            pltpu.VMEM((kv_heads, 2) + tile, BF16),
            pltpu.VMEM((kv_heads, 3) + tile, F32),
            pltpu.VMEM((kv_heads,) + tile, BF16),
            pltpu.VMEM((kv_heads,) + tile, BF16),
            pltpu.VMEM((kv_heads,) + tile, BF16),
            pltpu.VMEM((kv_heads,) + tile, BF16),
            pltpu.VMEM((3, rows, width), BF16),
            pltpu.VMEM(args[9].shape, jnp.int32),
            pltpu.VMEM(args[7].shape, jnp.int32),
            pltpu.VMEM(args[3].shape, jnp.int32),
            pltpu.VMEM((kv_heads, HEAD_DIM, GROUP * HEAD_DIM), F32),
            pltpu.VMEM((2, BLOCKS * HEAD_DIM, HEAD_DIM), F32),
            pltpu.VMEM((8, 128), F32),
            pltpu.VMEM((n_seq, 8, 128), F32),
            pltpu.VMEM((8, 128), F32),
            pltpu.VMEM((n_fsdp, 8, 128), F32),
            pltpu.VMEM((8, 128), F32),
            pltpu.VMEM((8, 128), F32),
            dma((3,)),
            dma((3,)),
            dma((3, TURNS)),
            dma((3, chunks)),
            dma((3, BACK_TURNS)),
            dma((3, kv_heads)),
            dma((2,)),
            dma((n_seq,)),
            dma((n_fsdp,)),
            dma((n_fsdp,)),
            dma((n_seq,)),
        ],
        compiler_params=pltpu.CompilerParams(
            collective_id=0, has_side_effects=True, vmem_limit_bytes=60 * 1024 * 1024
        ),
    )(*args)
    return pl.pallas_call(
        write_out,
        out_shape=tuple(jax.ShapeDtypeStruct(x.shape, BF16) for x in (q, q, k, k)),
        in_specs=[anywhere] * 4,
        out_specs=(anywhere,) * 4,
        scratch_shapes=[dma((4,))],
        compiler_params=pltpu.CompilerParams(vmem_limit_bytes=8 * 1024 * 1024),
    )(*(pltpu.with_memory_space_constraint(x, pltpu.VMEM) for x in done))


def solution(mesh):
    both = P(("fsdp", "seq"), None)
    ids = P("fsdp", None)
    return jax.shard_map(
        functools.partial(body, mesh.shape["fsdp"], mesh.shape["seq"]),
        mesh=mesh,
        in_specs=(both, both, both, ids, both, both, both, ids, both, P("fsdp", "seq")),
        out_specs=(both,) * 4,
        check_vma=False,
    )
```
